32 devices in a mesh: dp: 1 (over z), tp: 4 (over y), ep: 8 (over x, core).
Axes of the slice: x: 4, y: 4, z: 1, core: 2. Of those that a mesh axis runs over, the one named last changes fastest.
The devices are a block of a 4x4x8 slice.
Arguments:
- hidden_in: bfloat16 [1024, 2048], P(('dp', 'ep'))
- positions: int32 [1024], P(('dp', 'ep'))
- expert_ids: int32 [1024, 2], P(('dp', 'ep'))
- k_cache: bfloat16 [1024, 16, 16, 128], P(('dp', 'ep'), None, 'tp')
- v_cache: bfloat16 [1024, 16, 16, 128], P(('dp', 'ep'), None, 'tp')
- norm_in: bfloat16 [2048], replicated
- norm_res: bfloat16 [2048], replicated
- norm_post: bfloat16 [2048], replicated
- w_q: bfloat16 [2048, 2048], P(None, 'tp')
- w_k: bfloat16 [2048, 2048], P(None, 'tp')
- w_v: bfloat16 [2048, 2048], P(None, 'tp')
- w_o: bfloat16 [2048, 2048], P('tp')
- w_gate: bfloat16 [2048, 2816], P(None, 'tp')
- w_up: bfloat16 [2048, 2816], P(None, 'tp')
- w_down: bfloat16 [2816, 2048], P('tp')
- w_router: bfloat16 [2048, 64], replicated
- e_gate: bfloat16 [64, 2048, 1408], P('ep', None, 'tp')
- e_up: bfloat16 [64, 2048, 1408], P('ep', None, 'tp')
- e_down: bfloat16 [64, 1408, 2048], P('ep', 'tp')
Outputs:
- output 1: bfloat16 [1024, 2048], P(('dp', 'ep'))
- output 2: bfloat16 [1024, 16, 16, 128], P(('dp', 'ep'), None, 'tp')
- output 3: bfloat16 [1024, 16, 16, 128], P(('dp', 'ep'), None, 'tp')
All inputs are finite; a program needn't handle non-finite values.
Results may differ from the reference program's by a relative error of at most 0.0135542.
Values are sent between devices in bfloat16 or wider.
A program may use at most 768 MiB of HBM per device.

```python
import jax
import jax.numpy as jnp
from jax import lax

TOKENS = 128
EP_SHARDS = 8
CACHE_LEN = 16
MODEL_DIM = 2048
Q_HEADS = 16
KV_HEADS = 16
HEAD_DIM = 128
DENSE_FF = 2816
EXPERTS = 64
EXPERT_FF = 1408
ROPE_BASE = 10000
BATCH = TOKENS * EP_SHARDS
NORM_EPS = 1e-5


def draw_routes(route_key):
    mean_count = 2 * TOKENS // EP_SHARDS
    local_count = EXPERTS // EP_SHARDS
    sub_keys = jax.random.split(route_key, 5)
    shard_perm = jax.random.permutation(sub_keys[0], EP_SHARDS)
    lift_count = jax.random.randint(sub_keys[1], (EP_SHARDS, EP_SHARDS // 2), 0, mean_count + 1)
    lift_count = lift_count.at[0, 0].set(mean_count)
    paired = jnp.stack([lift_count, -lift_count], axis=-1).reshape(EP_SHARDS, EP_SHARDS)
    counts = mean_count + paired[:, jnp.argsort(shard_perm)]
    bounds = jnp.cumsum(counts, axis=1)
    slot_ids = jnp.arange(2 * TOKENS)
    dest_sorted = jnp.sum((bounds[:, None, :] <= slot_ids[None, :, None]).astype(jnp.int32), axis=2)

    def shuffle_tokens(sub_key):
        return jax.random.permutation(sub_key, TOKENS)

    token_perm = jax.vmap(shuffle_tokens)(jax.random.split(sub_keys[2], EP_SHARDS))
    first_dest = jnp.take_along_axis(dest_sorted, token_perm, axis=1)
    second_dest = jnp.take_along_axis(dest_sorted, token_perm + TOKENS, axis=1)
    swap_flag = jax.random.randint(sub_keys[3], (EP_SHARDS, TOKENS), 0, 2) == 1
    dest_pair = jnp.stack([jnp.where(swap_flag, second_dest, first_dest), jnp.where(swap_flag, first_dest, second_dest)], axis=-1)
    within = jax.random.randint(sub_keys[4], (EP_SHARDS, TOKENS, 2), 0, local_count)
    return (dest_pair * local_count + within).reshape(BATCH, 2).astype(jnp.int32)


def draw_matrix(sub_key, mat_shape, fan_in, factor):
    return (jax.random.normal(sub_key, mat_shape, jnp.float32) * (factor * fan_in ** -0.5)).astype(jnp.bfloat16)


def draw_expert_stack(stack_key, fan_in, fan_out):
    def one_expert(sub_key):
        return draw_matrix(sub_key, (fan_in, fan_out), fan_in, 1.0)
    return lax.map(one_expert, jax.random.split(stack_key, EXPERTS))


def draw_gain(sub_key):
    return jax.random.uniform(sub_key, (MODEL_DIM,), jnp.float32, 0.5, 1.5).astype(jnp.bfloat16)


def setup_inputs(seed: int = 0, part: int = 0) -> dict:
    part_key = jax.random.fold_in(jax.random.key(seed), part)
    part_keys = jax.random.split(part_key, 5)
    weight_keys = jax.random.split(jax.random.key(seed + 1), 15)
    attn_width = Q_HEADS * HEAD_DIM
    kv_width = KV_HEADS * HEAD_DIM
    cache_shape = (BATCH, CACHE_LEN, KV_HEADS, HEAD_DIM)
    return {
        'hidden_in': jax.random.normal(part_keys[0], (BATCH, MODEL_DIM), jnp.float32).astype(jnp.bfloat16),
        'positions': jax.random.randint(part_keys[1], (BATCH,), CACHE_LEN // 2, CACHE_LEN).at[0].set(CACHE_LEN - 1).astype(jnp.int32),
        'expert_ids': draw_routes(part_keys[2]),
        'k_cache': jax.random.normal(part_keys[3], cache_shape, jnp.float32).astype(jnp.bfloat16),
        'v_cache': jax.random.normal(part_keys[4], cache_shape, jnp.float32).astype(jnp.bfloat16),
        'norm_in': draw_gain(weight_keys[0]),
        'norm_res': draw_gain(weight_keys[1]),
        'norm_post': draw_gain(weight_keys[2]),
        'w_q': draw_matrix(weight_keys[3], (MODEL_DIM, attn_width), MODEL_DIM, 1.0),
        'w_k': draw_matrix(weight_keys[4], (MODEL_DIM, kv_width), MODEL_DIM, 1.0),
        'w_v': draw_matrix(weight_keys[5], (MODEL_DIM, kv_width), MODEL_DIM, 1.0),
        'w_o': draw_matrix(weight_keys[6], (attn_width, MODEL_DIM), attn_width, 0.5 * CACHE_LEN ** 0.5),
        'w_gate': draw_matrix(weight_keys[7], (MODEL_DIM, DENSE_FF), MODEL_DIM, 1.0),
        'w_up': draw_matrix(weight_keys[8], (MODEL_DIM, DENSE_FF), MODEL_DIM, 1.0),
        'w_down': draw_matrix(weight_keys[9], (DENSE_FF, MODEL_DIM), DENSE_FF, 1.0),
        'w_router': draw_matrix(weight_keys[10], (MODEL_DIM, EXPERTS), MODEL_DIM, 1.0),
        'e_gate': draw_expert_stack(weight_keys[11], MODEL_DIM, EXPERT_FF),
        'e_up': draw_expert_stack(weight_keys[12], MODEL_DIM, EXPERT_FF),
        'e_down': draw_expert_stack(weight_keys[13], EXPERT_FF, MODEL_DIM),
    }


def rms_norm(values, gain_vec):
    wide_vals = values.astype(jnp.float32)
    inv_rms = lax.rsqrt(jnp.mean(wide_vals * wide_vals, axis=-1, keepdims=True) + NORM_EPS)
    return (wide_vals * inv_rms * gain_vec.astype(jnp.float32)).astype(jnp.bfloat16)


def rope_rotate(values, positions):
    half_dim = HEAD_DIM // 2
    inv_freq = 1.0 / (ROPE_BASE ** (jnp.arange(0, HEAD_DIM, 2, dtype=jnp.float32) / HEAD_DIM))
    angles = positions.astype(jnp.float32)[:, None] * inv_freq[None, :]
    cosine = jnp.cos(angles)[:, None, :]
    sine_part = jnp.sin(angles)[:, None, :]
    first_half = values[..., :half_dim]
    second_half = values[..., half_dim:]
    return jnp.concatenate([first_half * cosine - second_half * sine_part, second_half * cosine + first_half * sine_part], axis=-1)


def reference(hidden_in, positions, expert_ids, k_cache, v_cache, norm_in, norm_res, norm_post, w_q, w_k, w_v, w_o, w_gate, w_up, w_down, w_router, e_gate, e_up, e_down):
    group_size = Q_HEADS // KV_HEADS
    normed = rms_norm(hidden_in, norm_in)
    q_proj = jnp.dot(normed, w_q, preferred_element_type=jnp.float32).reshape(BATCH, Q_HEADS, HEAD_DIM)
    k_proj = jnp.dot(normed, w_k, preferred_element_type=jnp.float32).reshape(BATCH, KV_HEADS, HEAD_DIM)
    v_new = jnp.dot(normed, w_v, preferred_element_type=jnp.float32).astype(jnp.bfloat16).reshape(BATCH, KV_HEADS, HEAD_DIM)
    q_rot = rope_rotate(q_proj, positions).astype(jnp.bfloat16)
    k_rot = rope_rotate(k_proj, positions).astype(jnp.bfloat16)
    slot_hit = (jnp.arange(CACHE_LEN)[None, :] == positions[:, None])[:, :, None, None]
    k_out = jnp.where(slot_hit, k_rot[:, None], k_cache)
    v_out = jnp.where(slot_hit, v_new[:, None], v_cache)

    def attend_token(operands):
        q_tok, k_tok, v_tok, pos_tok = operands
        q_grp = q_tok.reshape(KV_HEADS, group_size, HEAD_DIM).astype(jnp.float32)
        scores = jnp.einsum('kgd,tkd->kgt', q_grp, k_tok.astype(jnp.float32)) * (HEAD_DIM ** -0.5)
        visible = jnp.arange(CACHE_LEN)[None, None, :] <= pos_tok
        attn_probs = jax.nn.softmax(jnp.where(visible, scores, -jnp.inf), axis=-1)
        attn_probs = attn_probs.astype(jnp.bfloat16).astype(jnp.float32)
        mixed_vals = jnp.einsum('kgt,tkd->kgd', attn_probs, v_tok.astype(jnp.float32))
        return mixed_vals.astype(jnp.bfloat16).reshape(Q_HEADS * HEAD_DIM)

    attn_mix = lax.map(attend_token, (q_rot, k_out, v_out, positions))
    hidden_mid = (hidden_in.astype(jnp.float32) + jnp.dot(attn_mix, w_o, preferred_element_type=jnp.float32)).astype(jnp.bfloat16)
    res_in = rms_norm(hidden_mid, norm_res)
    gate_val = jnp.dot(res_in, w_gate, preferred_element_type=jnp.float32)
    up_val = jnp.dot(res_in, w_up, preferred_element_type=jnp.float32)
    dense_out = jnp.dot((jax.nn.silu(gate_val) * up_val).astype(jnp.bfloat16), w_down, preferred_element_type=jnp.float32)
    moe_in = rms_norm(hidden_in, norm_post)
    gate_probs = jax.nn.softmax(jnp.dot(moe_in, w_router, preferred_element_type=jnp.float32), axis=-1)
    picked = jnp.take_along_axis(gate_probs, expert_ids, axis=1)
    route_wts = picked / jnp.sum(picked, axis=1, keepdims=True)

    def expert_token(operands):
        row_vec, id_pair, wt_pair = operands
        moe_sum = jnp.zeros((MODEL_DIM,), jnp.float32)
        for choice in range(2):
            expert = id_pair[choice]
            gate_e = jnp.dot(row_vec[None, :], e_gate[expert], preferred_element_type=jnp.float32)
            up_e = jnp.dot(row_vec[None, :], e_up[expert], preferred_element_type=jnp.float32)
            act_e = (jax.nn.silu(gate_e) * up_e).astype(jnp.bfloat16)
            moe_sum = moe_sum + wt_pair[choice] * jnp.dot(act_e, e_down[expert], preferred_element_type=jnp.float32)[0]
        return moe_sum

    moe_out = lax.map(expert_token, (moe_in, expert_ids, route_wts))
    hidden_out = (hidden_mid.astype(jnp.float32) + dense_out + moe_out).astype(jnp.bfloat16)
    return (hidden_out, k_out, v_out)
```

```python
import functools

import jax
import jax.numpy as jnp
import numpy as np
from jax import lax
from jax.experimental import pallas as pl
from jax.experimental.pallas import tpu as pltpu
from jax.sharding import PartitionSpec as P

NORM_EPS = 1e-5
ROPE_BASE = 10000.0
F32 = jnp.float32
BF16 = jnp.bfloat16
MESH = pl.DeviceIdType.MESH
ROWS = 256
ALIGN = 16


def rms_norm(values, gain_row):
    wide_vals = values.astype(F32)
    inv_rms = lax.rsqrt(jnp.mean(wide_vals * wide_vals, axis=-1, keepdims=True) + NORM_EPS)
    return (wide_vals * inv_rms * gain_row.astype(F32)).astype(BF16)


def dot_nn(a, b):
    return lax.dot_general(a, b, (((1,), (0,)), ((), ())), preferred_element_type=F32)


def dot_nt(a, b):
    return lax.dot_general(a, b, (((1,), (1,)), ((), ())), preferred_element_type=F32)


def lane_scan(values):
    lane = lax.broadcasted_iota(jnp.int32, values.shape, 1)
    step = 1
    while step < values.shape[1]:
        values = values + jnp.where(lane >= step, pltpu.roll(values, step, 1), 0)
        step *= 2
    return values


def row_scan(values):
    row = lax.broadcasted_iota(jnp.int32, values.shape, 0)
    step = 1
    while step < values.shape[0]:
        values = values + jnp.where(row >= step, pltpu.roll(values, step, 0), 0)
        step *= 2
    return values


def layer_kernel(
    n_tp, n_ep, ep_axis, tp_axis,
    x_ref, pos_row_ref, pos_smem, ids_ref, n_in_ref, n_res_ref, n_post_ref, w_router_ref, rope_ref,
    k_hbm, v_hbm, wq_hbm, wk_hbm, wv_hbm, wo_hbm, wg_hbm, wu_hbm, wd_hbm, eg_hbm, eu_hbm, ed_hbm,
    out_ref, k_out, v_out,
    eg, eu, ed, rows_all, meta, all_ids, part_q, part_in, h_q, c_buf, d_in, r1_in, r2_in, dense_q, fin_q, fin_in, out_q,
    sched_v, sched,
    w_sem, e_sem, ag_send, ag_recv, m_send, m_recv, i_send, i_recv, a_send, a_recv, h_send, h_recv, d_send, d_recv,
    r1_send, r1_recv, r2_send, r2_recv, f_send, f_recv, o_send, o_recv,
):
    tokens, dim = x_ref.shape
    quarter = dim // n_tp
    n_x = n_ep // 2
    half = tokens // 2
    n_local, width = eg.shape[0], eg.shape[1]
    cache_len, heads, head_dim = k_hbm.shape[1], k_hbm.shape[2], k_hbm.shape[3]
    n_blocks = n_ep
    all_rows = n_blocks * tokens
    n_sorted = -(-(4 * tokens + n_local * (ALIGN - 1)) // 128) * 128
    n_steps = n_local + 1
    dense_parts = wd_hbm.shape[0]

    ep = lax.axis_index(ep_axis)
    tp = lax.axis_index(tp_axis)
    chip = ep // 2
    core = ep % 2
    other = 1 - core
    right = (chip + 1) % n_x
    left = (chip + n_x - 1) % n_x
    far = (chip + 2) % n_x

    def on_ring(place):
        return {ep_axis: place * 2 + core}

    partner = {ep_axis: chip * 2 + other}

    def ep_peer(k):
        return {ep_axis: (ep + k) % n_ep}

    def tp_peer(k):
        return {tp_axis: (tp + k) % n_tp}

    def remote(src, dst, send_sem, recv_sem, device):
        return pltpu.make_async_remote_copy(
            src_ref=src, dst_ref=dst, send_sem=send_sem, recv_sem=recv_sem, device_id=device, device_id_type=MESH)

    def arrived(dst, recv_sem):
        remote(dst, dst, recv_sem, recv_sem, partner).wait_recv()

    def sent(src, send_sem):
        remote(src, src, send_sem, send_sem, partner).wait_send()

    low, high = pl.ds(0, half), pl.ds(half, half)

    def forward(index, place, rows):
        block = rows_all.at[core, place, rows]
        arrived(block, ag_recv.at[index])
        remote(block, block, ag_send.at[index + 6], ag_recv.at[index + 6], partner).start()

    def forward_first():
        forward(1, left, low)
        block = rows_all.at[core, left, low]
        remote(block, block, ag_send.at[5], ag_recv.at[5], on_ring(right)).start()
        forward(3, right, high)
        block = rows_all.at[core, right, high]
        remote(block, block, ag_send.at[6], ag_recv.at[6], on_ring(left)).start()

    barrier = pltpu.get_barrier_semaphore()
    for k in range(1, n_ep):
        pl.semaphore_signal(barrier, inc=1, device_id=ep_peer(k), device_id_type=MESH)
    for k in range(1, n_tp):
        pl.semaphore_signal(barrier, inc=1, device_id=tp_peer(k), device_id_type=MESH)

    def attention_phase(wq, wk, wv, wo, kc, vc, q_s, k_s, v_s, o_s):
        loads = [
            pltpu.make_async_copy(src, dst, w_sem.at[i])
            for i, (src, dst) in enumerate(
                ((wq_hbm, wq), (wk_hbm, wk), (wv_hbm, wv), (k_hbm, kc), (v_hbm, vc), (wo_hbm, wo)))
        ]
        for load in loads:
            load.start()

        moe_in = rms_norm(x_ref[...], n_post_ref[...])
        rows_all[core, chip] = moe_in
        logits = dot_nt(w_router_ref[...], moe_in)
        shifted = jnp.exp(logits - jnp.max(logits, axis=0, keepdims=True))
        probs = shifted / jnp.sum(shifted, axis=0, keepdims=True)
        expert_row = lax.broadcasted_iota(jnp.int32, probs.shape, 0)
        ids = ids_ref[...]
        picked = [
            jnp.sum(jnp.where(expert_row == ids[k:k + 1, :], probs, 0.0), axis=0, keepdims=True) for k in range(2)
        ]
        total = picked[0] + picked[1]
        meta[core * n_x + chip] = jnp.concatenate(
            [picked[0] / total, picked[1] / total, jnp.zeros((6, tokens), F32)], axis=0)
        all_ids[core * n_x + chip] = jnp.concatenate([ids, jnp.zeros((6, tokens), jnp.int32)], axis=0)

        pl.semaphore_wait(barrier, n_ep - 1 + n_tp - 1)
        own = rows_all.at[core, chip]
        sends = [
            remote(own.at[low], own.at[low], ag_send.at[1], ag_recv.at[1], on_ring(right)),
            remote(own.at[high], own.at[high], ag_send.at[3], ag_recv.at[3], on_ring(left)),
            remote(own.at[high], own.at[high], ag_send.at[2], ag_recv.at[2], on_ring(right)),
            remote(own.at[low], own.at[low], ag_send.at[4], ag_recv.at[4], on_ring(left)),
            remote(own, own, ag_send.at[0], ag_recv.at[0], partner),
        ]
        for k in range(1, n_ep):
            block = meta.at[core * n_x + chip]
            sends.append(remote(block, block, m_send.at[k - 1], m_recv.at[k - 1], ep_peer(k)))
            block = all_ids.at[core * n_x + chip]
            sends.append(remote(block, block, i_send.at[k - 1], i_recv.at[k - 1], ep_peer(k)))
        for send in sends:
            send.start()

        normed = rms_norm(x_ref[...], n_in_ref[...])
        pos_col = jnp.transpose(jnp.broadcast_to(pos_row_ref[...].astype(F32), (tokens, tokens)))
        cosine = jnp.zeros((tokens, head_dim), F32)
        sine = jnp.zeros((tokens, head_dim), F32)
        for p in range(cache_len):
            cosine = jnp.where(pos_col == float(p), rope_ref[p:p + 1, :], cosine)
            sine = jnp.where(pos_col == float(p), rope_ref[cache_len + p:cache_len + p + 1, :], sine)

        def rotated(values):
            return values * cosine + pltpu.roll(values, head_dim // 2, 1) * sine

        for load, weights, dest, turn in (
            (loads[0], wq, q_s, True), (loads[1], wk, k_s, True), (loads[2], wv, v_s, False)):
            load.wait()
            proj = dot_nn(normed, weights[...])
            for head in range(heads):
                values = proj[:, head * head_dim:(head + 1) * head_dim]
                values = rotated(values) if turn else values
                dest[:, head, :] = values.astype(BF16).astype(F32)

        for e in range(n_local):
            pltpu.make_async_copy(eg_hbm.at[e], eg.at[e], e_sem.at[0, e]).start()
            pltpu.make_async_copy(eu_hbm.at[e], eu.at[e], e_sem.at[1, e]).start()
            pltpu.make_async_copy(ed_hbm.at[e], ed.at[e], e_sem.at[2, e]).start()

        loads[3].wait()
        loads[4].wait()
        slot = lax.broadcasted_iota(jnp.int32, (cache_len, heads, head_dim), 0)
        slot_one = lax.broadcasted_iota(jnp.int32, (cache_len, heads, 1), 0)
        unroll = 4

        def attend(group, carry):
            for i in range(unroll):
                t = group * unroll + i
                at = pos_smem[t]
                keys = jnp.where(slot == at, k_s[t][None], kc[t].astype(F32))
                kc[t] = keys.astype(BF16)
                scores = jnp.sum(keys * q_s[t][None], axis=-1, keepdims=True) * (head_dim ** -0.5)
                scores = jnp.where(slot_one <= at, scores, -jnp.inf)
                weights = jnp.exp(scores - jnp.max(scores, axis=0, keepdims=True))
                weights = weights / jnp.sum(weights, axis=0, keepdims=True)
                weights = weights.astype(BF16).astype(F32)
                vals = jnp.where(slot == at, v_s[t][None], vc[t].astype(F32))
                vc[t] = vals.astype(BF16)
                visible_vals = jnp.where(slot <= at, vals, 0.0)
                o_s[t] = jnp.sum(weights * visible_vals, axis=0)
            return carry

        lax.fori_loop(0, tokens // unroll, attend, 0)
        stores = [pltpu.make_async_copy(kc, k_out, w_sem.at[6]), pltpu.make_async_copy(vc, v_out, w_sem.at[7])]
        for store in stores:
            store.start()

        forward_first()

        mixed = jnp.concatenate([o_s[:, head, :] for head in range(heads)], axis=1).astype(BF16)
        loads[5].wait()
        for q in range(n_tp):
            part_q[q] = dot_nn(mixed, wo[:, q * quarter:(q + 1) * quarter]).astype(BF16)
        for k in range(1, n_tp):
            send = remote(part_q.at[(tp + k) % n_tp], part_in.at[k - 1], a_send.at[k - 1], a_recv.at[k - 1], tp_peer(k))
            send.start()
        for store in stores:
            store.wait()

    pl.run_scoped(
        attention_phase,
        *[pltpu.VMEM((dim, heads * head_dim), BF16)] * 3,
        pltpu.VMEM((heads * head_dim, dim), BF16),
        *[pltpu.VMEM((tokens, cache_len, heads, head_dim), BF16)] * 2,
        *[pltpu.VMEM((tokens, heads, head_dim), F32)] * 4,
    )

    forward(2, left, high)
    forward(4, right, low)

    mine = pl.ds(pl.multiple_of(tp * quarter, quarter), quarter)
    for k in range(1, n_tp):
        arrived(part_in.at[k - 1], a_recv.at[k - 1])
    attn_sum = part_q[tp].astype(F32)
    for k in range(1, n_tp):
        attn_sum = attn_sum + part_in[k - 1].astype(F32)
    h_q[tp] = (x_ref[:, mine].astype(F32) + attn_sum).astype(BF16)
    for k in range(1, n_tp):
        remote(h_q.at[tp], h_q.at[tp], h_send.at[k - 1], h_recv.at[k - 1], tp_peer(k)).start()

    forward(5, far, low)
    forward(6, far, high)

    def expert_phase(xs, sort, unsort, z, ys, y_sorted, weight_sorted):
        for k in range(1, n_ep):
            source = (ep + n_ep - k) % n_ep
            arrived(meta.at[(source % 2) * n_x + source // 2], m_recv.at[k - 1])
            arrived(all_ids.at[(source % 2) * n_x + source // 2], i_recv.at[k - 1])
        ids = [all_ids[:, k, :] for k in range(2)]
        wts = [meta[:, k, :] for k in range(2)]
        first = ep * n_local
        lane = lax.broadcasted_iota(jnp.int32, (n_blocks, tokens), 1)
        start = jnp.zeros((n_blocks, tokens), jnp.int32)
        place = jnp.full((n_blocks, tokens), -1, jnp.int32)
        weight = jnp.zeros((n_blocks, tokens), F32)
        step_expert = jnp.zeros((n_blocks, tokens), jnp.int32)
        step_row = jnp.zeros((n_blocks, tokens), jnp.int32)
        block_row = jnp.zeros((n_blocks, tokens), jnp.int32)
        for e in range(n_local):
            here = [i == first + e for i in ids]
            hit = jnp.where(jnp.logical_or(here[0], here[1]), 1, 0)
            weight = jnp.where(here[0], wts[0], jnp.where(here[1], wts[1], weight))
            scan = lane_scan(hit)
            totals = jnp.broadcast_to(scan[:, tokens - 1:], scan.shape)
            above = row_scan(totals)
            count = jnp.broadcast_to(above[n_blocks - 1:, :], scan.shape)
            place = jnp.where(hit == 1, start + above - totals + scan - 1, place)
            step_row = jnp.where(lane == e, start, step_row)
            step_expert = jnp.where(lane == e, e, step_expert)
            spill = jnp.logical_and(lane == n_local, count > ROWS)
            step_row = jnp.where(spill, start + ROWS, step_row)
            step_expert = jnp.where(spill, e, step_expert)
            later = start + (count + ALIGN - 1) // ALIGN * ALIGN
            into = lane * ALIGN - start
            inside = jnp.logical_and(into >= 0, lane * ALIGN < later)
            block_row = jnp.where(
                inside, jnp.where(into < ROWS, e * ROWS + into, n_local * ROWS + into - ROWS), block_row)
            start = later
        step_row = jnp.minimum(step_row, n_sorted)
        block_row = jnp.minimum(block_row, n_steps * ROWS - ALIGN)
        table_row = lax.broadcasted_iota(jnp.int32, (n_blocks, tokens), 0)
        sched_v[...] = jnp.where(
            table_row == 0, step_expert, jnp.where(table_row == 1, step_row // ALIGN, block_row // ALIGN))
        to_scalar = pltpu.make_async_copy(sched_v, sched, w_sem.at[8])
        to_scalar.start()

        row_id = lax.broadcasted_iota(jnp.int32, (n_sorted, tokens), 0)
        weight_rows = jnp.zeros((n_sorted, tokens), F32)
        for j in range(n_blocks):
            match = row_id == place[j:j + 1, :]
            sort[:, j * tokens:(j + 1) * tokens] = jnp.where(match, 1.0, 0.0).astype(BF16)
            weight_rows = weight_rows + jnp.where(match, weight[j:j + 1, :], 0.0)
        weight_sorted[0:n_sorted, :] = jnp.broadcast_to(
            jnp.sum(weight_rows, axis=1, keepdims=True), (n_sorted, 128))
        weight_sorted[n_sorted:, :] = jnp.zeros((ROWS, 128), F32)
        xs[n_sorted:, :] = jnp.zeros((ROWS, dim), BF16)
        place_cols = jnp.transpose(place.astype(F32))
        column_id = lax.broadcasted_iota(jnp.int32, (tokens, n_sorted), 1).astype(F32)
        for j in range(n_blocks):
            unsort[j * tokens:(j + 1) * tokens, :] = jnp.where(
                column_id == place_cols[:, j:j + 1], 1.0, 0.0).astype(BF16)

        arrived(rows_all.at[other, chip], ag_recv.at[0])
        for index, spot, part in ((1, left, low), (2, left, high), (3, right, high), (4, right, low), (5, far, low), (6, far, high)):
            arrived(rows_all.at[other, spot, part], ag_recv.at[index + 6])
        for index in range(1, 13):
            sent(rows_all.at[core, chip, low], ag_send.at[index])
        sent(rows_all.at[core, chip], ag_send.at[0])
        for k in range(1, n_ep):
            sent(meta.at[core * n_x + chip], m_send.at[k - 1])
            sent(all_ids.at[core * n_x + chip], i_send.at[k - 1])

        def sort_columns(i, carry):
            cols = pl.ds(pl.multiple_of(i * 256, 256), 256)
            rows = rows_all[:, :, :, cols].reshape(all_rows, 256)
            xs[0:n_sorted, cols] = dot_nn(sort[...], rows).astype(BF16)
            return carry

        lax.fori_loop(0, dim // 256, sort_columns, 0)
        to_scalar.wait()
        for e in range(n_local):
            pltpu.make_async_copy(eg_hbm.at[e], eg.at[e], e_sem.at[0, e]).wait()
            pltpu.make_async_copy(eu_hbm.at[e], eu.at[e], e_sem.at[1, e]).wait()

        def gate_up(step, carry):
            e = sched[0, step]
            rows = xs[pl.ds(sched[1, step] * ALIGN, ROWS), :]
            act = jax.nn.silu(dot_nt(eg[e], rows)) * dot_nt(eu[e], rows)
            z[step] = jnp.transpose(act).astype(BF16)
            return carry

        lax.fori_loop(0, n_steps, gate_up, 0)

        for p in range(dense_parts):
            pltpu.make_async_copy(wg_hbm.at[p], eg.at[p], w_sem.at[p]).start()
            pltpu.make_async_copy(wu_hbm.at[p], eu.at[p], w_sem.at[2 + p]).start()
            pltpu.make_async_copy(wd_hbm.at[p], eg.at[dense_parts + p], w_sem.at[4 + p]).start()
        for e in range(n_local):
            pltpu.make_async_copy(ed_hbm.at[e], ed.at[e], e_sem.at[2, e]).wait()

        for i in range(n_tp):
            cols = columns(i)

            def down(step, carry):
                e = sched[0, step]
                scale = weight_sorted[pl.ds(sched[1, step] * ALIGN, ROWS), :]
                prod = dot_nn(z[step], ed[e, :, cols])
                scaled = [prod[:, b * 128:(b + 1) * 128] * scale for b in range(quarter // 128)]
                ys[pl.ds(pl.multiple_of(step * ROWS, ROWS), ROWS), :] = jnp.concatenate(scaled, axis=1).astype(BF16)
                return carry

            lax.fori_loop(0, n_steps, down, 0)

            def regroup(b, carry):
                y_sorted[pl.ds(pl.multiple_of(b * ALIGN, ALIGN), ALIGN), :] = ys[
                    pl.ds(sched[2, b] * ALIGN, ALIGN), :]
                return carry

            lax.fori_loop(0, n_sorted // ALIGN, regroup, 0)
            for c in range(2):
                back = dot_nn(unsort[c * n_x * tokens:(c + 1) * n_x * tokens, :], y_sorted[...])
                rows_all[c, :, :, cols] = back.astype(BF16).reshape(n_x, tokens, quarter)
            remote(rows_all.at[other, :, :, cols], d_in.at[i], d_send.at[i], d_recv.at[i], partner).start()
            if i >= 1:
                pair_sum(i - 1)
            if i >= 2:
                ring_sum(i - 2)

    def columns(i):
        return pl.ds(pl.multiple_of(((tp + 1 + i) % n_tp) * quarter, quarter), quarter)

    def pair_sum(i):
        cols = columns(i)
        arrived(d_in.at[i], d_recv.at[i])
        for spot in range(n_x):
            rows_all[core, spot, :, cols] = (
                rows_all[core, spot, :, cols].astype(F32) + d_in[i, spot].astype(F32)).astype(BF16)
        remote(rows_all.at[core, far, low, cols], r1_in.at[i, 0], r1_send.at[i, 0], r1_recv.at[i, 0], on_ring(right)).start()
        remote(rows_all.at[core, far, high, cols], r1_in.at[i, 1], r1_send.at[i, 1], r1_recv.at[i, 1], on_ring(left)).start()
        remote(rows_all.at[core, right, high, cols], r2_in.at[i, 0, high], r2_send.at[i, 0], r2_recv.at[i, 0], on_ring(right)).start()
        remote(rows_all.at[core, left, low, cols], r2_in.at[i, 1, low], r2_send.at[i, 1], r2_recv.at[i, 1], on_ring(left)).start()

    def ring_sum(i):
        cols = columns(i)
        arrived(r1_in.at[i, 0], r1_recv.at[i, 0])
        rows_all[core, right, low, cols] = (
            rows_all[core, right, low, cols].astype(F32) + r1_in[i, 0].astype(F32)).astype(BF16)
        remote(rows_all.at[core, right, low, cols], r2_in.at[i, 0, low], r2_send.at[i, 2], r2_recv.at[i, 2], on_ring(right)).start()
        arrived(r1_in.at[i, 1], r1_recv.at[i, 1])
        rows_all[core, left, high, cols] = (
            rows_all[core, left, high, cols].astype(F32) + r1_in[i, 1].astype(F32)).astype(BF16)
        remote(rows_all.at[core, left, high, cols], r2_in.at[i, 1, high], r2_send.at[i, 3], r2_recv.at[i, 3], on_ring(left)).start()

    pl.run_scoped(
        expert_phase,
        pltpu.VMEM((n_sorted + ROWS, dim), BF16),
        pltpu.VMEM((n_sorted, all_rows), BF16),
        pltpu.VMEM((all_rows, n_sorted), BF16),
        pltpu.VMEM((n_steps, ROWS, width), BF16),
        pltpu.VMEM((n_steps * ROWS, quarter), BF16),
        pltpu.VMEM((n_sorted, quarter), BF16),
        pltpu.VMEM((n_sorted + ROWS, 128), F32),
    )
    pair_sum(n_tp - 1)
    ring_sum(n_tp - 2)

    for k in range(1, n_tp):
        source = (tp + n_tp - k) % n_tp
        arrived(h_q.at[source], h_recv.at[k - 1])
    hidden_mid = jnp.concatenate([h_q[q] for q in range(n_tp)], axis=1)
    c_buf[...] = rms_norm(hidden_mid, n_res_ref[...])
    acts = []
    for p in range(dense_parts):
        pltpu.make_async_copy(wg_hbm.at[p], eg.at[p], w_sem.at[p]).wait()
        pltpu.make_async_copy(wu_hbm.at[p], eu.at[p], w_sem.at[2 + p]).wait()
        act = jax.nn.silu(dot_nt(eg[p], c_buf[...])) * dot_nt(eu[p], c_buf[...])
        acts.append(jnp.transpose(act).astype(BF16))
    for p in range(dense_parts):
        pltpu.make_async_copy(wd_hbm.at[p], eg.at[dense_parts + p], w_sem.at[4 + p]).wait()
    for q in range(n_tp):
        cols = slice(q * quarter, (q + 1) * quarter)
        dense = dot_nn(acts[0], eg[dense_parts, :, cols])
        for p in range(1, dense_parts):
            dense = dense + dot_nn(acts[p], eg[dense_parts + p, :, cols])
        dense_q[q] = dense
    ring_sum(n_tp - 1)

    for i in range(n_tp):
        q = (tp + 1 + i) % n_tp
        cols = columns(i)
        arrived(r2_in.at[i, 0, high], r2_recv.at[i, 0])
        arrived(r2_in.at[i, 1, low], r2_recv.at[i, 1])
        arrived(r2_in.at[i, 0, low], r2_recv.at[i, 2])
        arrived(r2_in.at[i, 1, high], r2_recv.at[i, 3])
        part = rows_all[core, chip, :, cols].astype(F32) + r2_in[i, 0].astype(F32) + r2_in[i, 1].astype(F32) + dense_q[q]
        if i < n_tp - 1:
            fin_q[i] = part.astype(BF16)
            remote(fin_q.at[i], fin_in.at[i], f_send.at[i], f_recv.at[i], tp_peer(i + 1)).start()
        else:
            for k in range(1, n_tp):
                arrived(fin_in.at[k - 1], f_recv.at[k - 1])
                part = part + fin_in[k - 1].astype(F32)
            out_q[tp] = (h_q[tp].astype(F32) + part).astype(BF16)
    for k in range(1, n_tp):
        remote(out_q.at[tp], out_q.at[tp], o_send.at[k - 1], o_recv.at[k - 1], tp_peer(k)).start()

    for i in range(n_tp):
        cols = columns(i)
        sent(d_in.at[i], d_send.at[i])
        for side in range(2):
            sent(r1_in.at[i, side], r1_send.at[i, side])
        for message in range(4):
            sent(r1_in.at[i, 0], r2_send.at[i, message])
    for k in range(1, n_tp):
        sent(part_in.at[k - 1], a_send.at[k - 1])
        sent(part_in.at[k - 1], h_send.at[k - 1])
        sent(part_in.at[k - 1], f_send.at[k - 1])
    for k in range(1, n_tp):
        source = (tp + n_tp - k) % n_tp
        arrived(out_q.at[source], o_recv.at[k - 1])
    for q in range(n_tp):
        out_ref[:, q * quarter:(q + 1) * quarter] = out_q[q]
    for k in range(1, n_tp):
        sent(part_in.at[k - 1], o_send.at[k - 1])


def rope_table(cache_len, head_dim):
    freq = 1.0 / (ROPE_BASE ** (np.arange(0, head_dim, 2, dtype=np.float32) / np.float32(head_dim)))
    angle = np.arange(cache_len, dtype=np.float32)[:, None] * freq.astype(np.float32)[None, :]
    cosine, sine = np.cos(angle), np.sin(angle)
    return np.concatenate(
        [np.concatenate([cosine, cosine], 1), np.concatenate([-sine, sine], 1)], 0).astype(np.float32)


def solution(mesh):
    n_tp, n_ep = mesh.shape['tp'], mesh.shape['ep']
    row_spec = P(('dp', 'ep'), None)
    cache_spec = P(('dp', 'ep'), None, 'tp', None)
    col_split = P(None, 'tp')
    row_split = P('tp', None)
    in_specs = (row_spec, P(('dp', 'ep')), row_spec, cache_spec, cache_spec, P(None), P(None), P(None), col_split, col_split, col_split, row_split, col_split, col_split, row_split, P(None, None), P('ep', None, 'tp'), P('ep', None, 'tp'), P('ep', 'tp', None))
    out_specs = (row_spec, cache_spec, cache_spec)

    def local_layer(hidden_in, positions, expert_ids, k_cache, v_cache, norm_in, norm_res, norm_post, w_q, w_k, w_v, w_o, w_gate, w_up, w_down, w_router, e_gate, e_up, e_down):
        tokens, dim = hidden_in.shape
        n_local, width = e_gate.shape[0], e_gate.shape[2]
        cache_len, head_dim = k_cache.shape[1], k_cache.shape[3]
        dense_parts = w_down.shape[0] // width
        quarter = dim // n_tp
        n_x = n_ep // 2
        half = tokens // 2
        vmem = pl.BlockSpec(memory_space=pltpu.VMEM)
        hbm = pl.BlockSpec(memory_space=pl.ANY)
        dma = pltpu.SemaphoreType.DMA
        return pl.pallas_call(
            functools.partial(layer_kernel, n_tp, n_ep, 'ep', 'tp'),
            out_shape=(
                jax.ShapeDtypeStruct(hidden_in.shape, BF16),
                jax.ShapeDtypeStruct(k_cache.shape, BF16),
                jax.ShapeDtypeStruct(v_cache.shape, BF16),
            ),
            in_specs=[vmem, vmem, pl.BlockSpec(memory_space=pltpu.SMEM)] + [vmem] * 6 + [hbm] * 12,
            out_specs=(vmem, hbm, hbm),
            scratch_shapes=[
                pltpu.VMEM((n_local, width, dim), BF16),
                pltpu.VMEM((n_local, width, dim), BF16),
                pltpu.VMEM((n_local, width, dim), BF16),
                pltpu.VMEM((2, n_x, tokens, dim), BF16),
                pltpu.VMEM((n_ep, 8, tokens), F32),
                pltpu.VMEM((n_ep, 8, tokens), jnp.int32),
                pltpu.VMEM((n_tp, tokens, quarter), BF16),
                pltpu.VMEM((n_tp - 1, tokens, quarter), BF16),
                pltpu.VMEM((n_tp, tokens, quarter), BF16),
                pltpu.VMEM((tokens, dim), BF16),
                pltpu.VMEM((n_tp, n_x, tokens, quarter), BF16),
                pltpu.VMEM((n_tp, 2, half, quarter), BF16),
                pltpu.VMEM((n_tp, 2, tokens, quarter), BF16),
                pltpu.VMEM((n_tp, tokens, quarter), F32),
                pltpu.VMEM((n_tp - 1, tokens, quarter), BF16),
                pltpu.VMEM((n_tp - 1, tokens, quarter), BF16),
                pltpu.VMEM((n_tp, tokens, quarter), BF16),
                pltpu.VMEM((n_ep, tokens), jnp.int32),
                pltpu.SMEM((n_ep, tokens), jnp.int32),
                dma((9,)), dma((3, n_local)), dma((13,)), dma((13,)), *[dma((n_ep - 1,))] * 4,
                *[dma((n_tp - 1,))] * 4,
                dma((n_tp,)), dma((n_tp,)),
                dma((n_tp, 2)), dma((n_tp, 2)), dma((n_tp, 4)), dma((n_tp, 4)),
                *[dma((n_tp - 1,))] * 4,
            ],
            compiler_params=pltpu.CompilerParams(
                collective_id=0, has_side_effects=True, vmem_limit_bytes=67043328),
        )(
            hidden_in, positions.reshape(1, tokens), positions, expert_ids.T,
            norm_in.reshape(1, dim), norm_res.reshape(1, dim), norm_post.reshape(1, dim), w_router.T,
            jnp.asarray(rope_table(cache_len, head_dim)),
            k_cache, v_cache, w_q, w_k, w_v, w_o,
            w_gate.T.reshape(dense_parts, width, dim), w_up.T.reshape(dense_parts, width, dim),
            w_down.reshape(dense_parts, width, dim),
            jnp.swapaxes(e_gate, 1, 2), jnp.swapaxes(e_up, 1, 2), e_down,
        )

    return jax.shard_map(local_layer, mesh=mesh, in_specs=in_specs, out_specs=out_specs, check_vma=False)
```

```python
import functools

import jax
import jax.numpy as jnp
import numpy as np
from jax import lax
from jax.experimental import pallas as pl
from jax.experimental.pallas import tpu as pltpu
from jax.sharding import PartitionSpec as P

NORM_EPS = 1e-5
ROPE_BASE = 10000.0
F32 = jnp.float32
BF16 = jnp.bfloat16
MESH = pl.DeviceIdType.MESH
ROWS = 256
ALIGN = 16


def as_row(gains):
    wide = gains.astype(F32)
    return jnp.concatenate([wide[i:i + 1, :] for i in range(wide.shape[0])], axis=1)


def rms_norm(values, gain_row):
    wide_vals = values.astype(F32)
    inv_rms = lax.rsqrt(jnp.mean(wide_vals * wide_vals, axis=-1, keepdims=True) + NORM_EPS)
    return (wide_vals * inv_rms * gain_row.astype(F32)).astype(BF16)


def dot_nn(a, b):
    return lax.dot_general(a, b, (((1,), (0,)), ((), ())), preferred_element_type=F32)


def dot_nt(a, b):
    return lax.dot_general(a, b, (((1,), (1,)), ((), ())), preferred_element_type=F32)


def lane_scan(values):
    lane = lax.broadcasted_iota(jnp.int32, values.shape, 1)
    step = 1
    while step < values.shape[1]:
        values = values + jnp.where(lane >= step, pltpu.roll(values, step, 1), 0)
        step *= 2
    return values


def row_scan(values):
    row = lax.broadcasted_iota(jnp.int32, values.shape, 0)
    step = 1
    while step < values.shape[0]:
        values = values + jnp.where(row >= step, pltpu.roll(values, step, 0), 0)
        step *= 2
    return values


def layer_kernel(
    n_tp, n_ep, ep_axis, tp_axis,
    x_ref, pos_row_ref, ids_ref, n_in_ref, n_res_ref, n_post_ref, w_router_ref, rope_ref,
    k_hbm, v_hbm, wq_hbm, wk_hbm, wv_hbm, wo_hbm, wg_hbm, wu_hbm, wd_hbm, eg_hbm, eu_hbm, ed_hbm,
    out_ref, k_new, v_new,
    eg, eu, ed, rows_all, meta, all_ids, part_q, part_in, h_q, c_buf, d_in, r1_in, r2_in, dense_q, fin_q, fin_in, out_q,
    sched_v, sched,
    w_sem, e_sem, ag_send, ag_recv, m_send, m_recv, i_send, i_recv, a_send, a_recv, h_send, h_recv, d_send, d_recv,
    r1_send, r1_recv, r2_send, r2_recv, f_send, f_recv, o_send, o_recv,
):
    tokens, dim = x_ref.shape
    quarter = dim // n_tp
    n_x = n_ep // 2
    half = tokens // 2
    n_local, width = eg.shape[0], eg.shape[1]
    head_dim = k_hbm.shape[1]
    heads = wq_hbm.shape[1] // head_dim
    cache_len = k_hbm.shape[0] // (tokens * heads)
    n_blocks = n_ep
    all_rows = n_blocks * tokens
    n_sorted = -(-(4 * tokens + n_local * (ALIGN - 1)) // 128) * 128
    n_steps = n_local + 1
    dense_parts = wd_hbm.shape[0]

    ep = lax.axis_index(ep_axis)
    tp = lax.axis_index(tp_axis)
    chip = ep // 2
    core = ep % 2
    other = 1 - core
    right = (chip + 1) % n_x
    left = (chip + n_x - 1) % n_x
    far = (chip + 2) % n_x

    def on_ring(place):
        return {ep_axis: place * 2 + core}

    partner = {ep_axis: chip * 2 + other}

    def ep_peer(k):
        return {ep_axis: (ep + k) % n_ep}

    def tp_peer(k):
        return {tp_axis: (tp + k) % n_tp}

    def remote(src, dst, send_sem, recv_sem, device):
        return pltpu.make_async_remote_copy(
            src_ref=src, dst_ref=dst, send_sem=send_sem, recv_sem=recv_sem, device_id=device, device_id_type=MESH)

    def arrived(dst, recv_sem):
        remote(dst, dst, recv_sem, recv_sem, partner).wait_recv()

    def sent(src, send_sem):
        remote(src, src, send_sem, send_sem, partner).wait_send()

    low, high = pl.ds(0, half), pl.ds(half, half)

    def forward(index, place, rows):
        block = rows_all.at[core, place, rows]
        arrived(block, ag_recv.at[index])
        remote(block, block, ag_send.at[index + 6], ag_recv.at[index + 6], partner).start()

    def forward_first():
        forward(1, left, low)
        block = rows_all.at[core, left, low]
        remote(block, block, ag_send.at[5], ag_recv.at[5], on_ring(right)).start()
        forward(3, right, high)
        block = rows_all.at[core, right, high]
        remote(block, block, ag_send.at[6], ag_recv.at[6], on_ring(left)).start()

    barrier = pltpu.get_barrier_semaphore()
    for k in range(1, n_ep):
        pl.semaphore_signal(barrier, inc=1, device_id=ep_peer(k), device_id_type=MESH)
    for k in range(1, n_tp):
        pl.semaphore_signal(barrier, inc=1, device_id=tp_peer(k), device_id_type=MESH)

    def attention_phase(wq, wk, wv, wo, kc, vc, q_s, k_s, v_s, o_s, pos_s):
        loads = [
            pltpu.make_async_copy(src, dst, w_sem.at[i])
            for i, (src, dst) in enumerate(
                ((wq_hbm, wq), (wk_hbm, wk), (wv_hbm, wv), (k_hbm, kc), (v_hbm, vc), (wo_hbm, wo)))
        ]
        for load in loads:
            load.start()

        moe_in = rms_norm(x_ref[...], as_row(n_post_ref[...]))
        rows_all[core, chip] = moe_in
        logits = dot_nt(w_router_ref[...], moe_in)
        shifted = jnp.exp(logits - jnp.max(logits, axis=0, keepdims=True))
        probs = shifted / jnp.sum(shifted, axis=0, keepdims=True)
        expert_row = lax.broadcasted_iota(jnp.int32, probs.shape, 0)
        ids = ids_ref[...]
        picked = [
            jnp.sum(jnp.where(expert_row == ids[k:k + 1, :], probs, 0.0), axis=0, keepdims=True) for k in range(2)
        ]
        total = picked[0] + picked[1]
        meta[core * n_x + chip] = jnp.concatenate(
            [picked[0] / total, picked[1] / total, jnp.zeros((6, tokens), F32)], axis=0)
        all_ids[core * n_x + chip] = jnp.concatenate([ids, jnp.zeros((6, tokens), jnp.int32)], axis=0)

        pl.semaphore_wait(barrier, n_ep - 1 + n_tp - 1)
        own = rows_all.at[core, chip]
        sends = [
            remote(own.at[low], own.at[low], ag_send.at[1], ag_recv.at[1], on_ring(right)),
            remote(own.at[high], own.at[high], ag_send.at[3], ag_recv.at[3], on_ring(left)),
            remote(own.at[high], own.at[high], ag_send.at[2], ag_recv.at[2], on_ring(right)),
            remote(own.at[low], own.at[low], ag_send.at[4], ag_recv.at[4], on_ring(left)),
            remote(own, own, ag_send.at[0], ag_recv.at[0], partner),
        ]
        for k in range(1, n_ep):
            block = meta.at[core * n_x + chip]
            sends.append(remote(block, block, m_send.at[k - 1], m_recv.at[k - 1], ep_peer(k)))
            block = all_ids.at[core * n_x + chip]
            sends.append(remote(block, block, i_send.at[k - 1], i_recv.at[k - 1], ep_peer(k)))
        for send in sends:
            send.start()

        normed = rms_norm(x_ref[...], as_row(n_in_ref[...]))
        pos_col = jnp.transpose(jnp.broadcast_to(pos_row_ref[...].astype(F32), (tokens, tokens)))
        cosine = jnp.zeros((tokens, head_dim), F32)
        sine = jnp.zeros((tokens, head_dim), F32)
        for p in range(cache_len):
            cosine = jnp.where(pos_col == float(p), rope_ref[p:p + 1, :], cosine)
            sine = jnp.where(pos_col == float(p), rope_ref[cache_len + p:cache_len + p + 1, :], sine)

        def rotated(values):
            return values * cosine + pltpu.roll(values, head_dim // 2, 1) * sine

        for head in range(heads):
            pos_s[pl.ds(head, tokens, stride=heads), :] = pos_col
        for load, weights, dest in ((loads[0], wq, q_s), (loads[1], wk, k_s), (loads[2], wv, v_s)):
            load.wait()
            proj = dot_nn(normed, weights[...])
            for head in range(heads):
                values = proj[:, head * head_dim:(head + 1) * head_dim]
                if dest is not v_s:
                    values = rotated(values)
                dest[pl.ds(head, tokens, stride=heads), :] = values.astype(BF16).astype(F32)
        k_new[...] = k_s[...].astype(BF16)
        v_new[...] = v_s[...].astype(BF16)

        for e in range(n_local):
            pltpu.make_async_copy(eg_hbm.at[e], eg.at[e], e_sem.at[0, e]).start()
            pltpu.make_async_copy(eu_hbm.at[e], eu.at[e], e_sem.at[1, e]).start()
            pltpu.make_async_copy(ed_hbm.at[e], ed.at[e], e_sem.at[2, e]).start()

        loads[3].wait()
        loads[4].wait()
        group = 16 // heads
        q_rows, slots = 16, group * cache_len * heads
        shape = (q_rows, slots)
        row, col = lax.broadcasted_iota(jnp.int32, shape, 0), lax.broadcasted_iota(jnp.int32, shape, 1)
        own_rows = jnp.logical_and(row // heads == col // (cache_len * heads), row % heads == col % heads)
        slot = jnp.where(own_rows, col // heads % cache_len, cache_len).astype(F32)

        def attend(g, carry):
            rows = pl.ds(pl.multiple_of(g * q_rows, q_rows), q_rows)
            wide_rows = pl.ds(pl.multiple_of(g * slots, slots), slots)
            query, key = q_s[rows, :], k_s[rows, :]
            at = pos_s[rows, :]
            scores = dot_nt(query.astype(BF16), kc[wide_rows, :]) * (head_dim ** -0.5)
            scores = jnp.where(slot < jnp.concatenate([at] * (slots // 128), axis=1), scores, -jnp.inf)
            score_new = jnp.sum(query * key, axis=1, keepdims=True) * (head_dim ** -0.5)
            top = jnp.maximum(jnp.max(scores, axis=1, keepdims=True), score_new)
            weights, weight_new = jnp.exp(scores - top), jnp.exp(score_new - top)
            total = jnp.sum(weights, axis=1, keepdims=True) + weight_new
            mix = dot_nn((weights / total).astype(BF16), vc[wide_rows, :])
            o_s[rows, :] = mix + (weight_new / total).astype(BF16).astype(F32) * v_s[rows, :]
            return carry

        lax.fori_loop(0, tokens // group, attend, 0, unroll=8)

        forward_first()

        mixed = jnp.concatenate(
            [o_s[pl.ds(head, tokens, stride=heads), :] for head in range(heads)], axis=1).astype(BF16)
        loads[5].wait()
        for q in range(n_tp):
            part_q[q] = dot_nn(mixed, wo[:, q * quarter:(q + 1) * quarter]).astype(BF16)
        for k in range(1, n_tp):
            send = remote(part_q.at[(tp + k) % n_tp], part_in.at[k - 1], a_send.at[k - 1], a_recv.at[k - 1], tp_peer(k))
            send.start()

    pl.run_scoped(
        attention_phase,
        *[pltpu.VMEM((dim, heads * head_dim), BF16)] * 3,
        pltpu.VMEM((heads * head_dim, dim), BF16),
        *[pltpu.VMEM(k_hbm.shape, BF16)] * 2,
        *[pltpu.VMEM((tokens * heads, head_dim), F32)] * 5,
    )

    def attention_sum():
        mine = pl.ds(pl.multiple_of(tp * quarter, quarter), quarter)
        for k in range(1, n_tp):
            arrived(part_in.at[k - 1], a_recv.at[k - 1])
        attn_sum = part_q[tp].astype(F32)
        for k in range(1, n_tp):
            attn_sum = attn_sum + part_in[k - 1].astype(F32)
        h_q[tp] = (x_ref[:, mine].astype(F32) + attn_sum).astype(BF16)
        for k in range(1, n_tp):
            remote(h_q.at[tp], h_q.at[tp], h_send.at[k - 1], h_recv.at[k - 1], tp_peer(k)).start()

    def expert_phase(xs, sort, unsort, z, ys, y_sorted, weight_sorted, place_s, weight_s, act_s):
        for k in range(1, n_ep):
            source = (ep + n_ep - k) % n_ep
            arrived(meta.at[(source % 2) * n_x + source // 2], m_recv.at[k - 1])
            arrived(all_ids.at[(source % 2) * n_x + source // 2], i_recv.at[k - 1])
        ids = [all_ids[:, k, :] for k in range(2)]
        wts = [meta[:, k, :] for k in range(2)]
        first = ep * n_local
        lane = lax.broadcasted_iota(jnp.int32, (n_blocks, tokens), 1)
        start = jnp.zeros((n_blocks, tokens), jnp.int32)
        place = jnp.full((n_blocks, tokens), -1, jnp.int32)
        weight = jnp.zeros((n_blocks, tokens), F32)
        step_expert = jnp.zeros((n_blocks, tokens), jnp.int32)
        step_row = jnp.zeros((n_blocks, tokens), jnp.int32)
        block_row = jnp.zeros((n_blocks, tokens), jnp.int32)
        for e in range(n_local):
            here = [i == first + e for i in ids]
            hit = jnp.where(jnp.logical_or(here[0], here[1]), 1, 0)
            weight = jnp.where(here[0], wts[0], jnp.where(here[1], wts[1], weight))
            scan = lane_scan(hit)
            totals = jnp.broadcast_to(scan[:, tokens - 1:], scan.shape)
            above = row_scan(totals)
            count = jnp.broadcast_to(above[n_blocks - 1:, :], scan.shape)
            place = jnp.where(hit == 1, start + above - totals + scan - 1, place)
            step_row = jnp.where(lane == e, start, step_row)
            step_expert = jnp.where(lane == e, e, step_expert)
            spill = jnp.logical_and(lane == n_local, count > ROWS)
            step_row = jnp.where(spill, start + ROWS, step_row)
            step_expert = jnp.where(spill, e, step_expert)
            later = start + (count + ALIGN - 1) // ALIGN * ALIGN
            into = lane * ALIGN - start
            inside = jnp.logical_and(into >= 0, lane * ALIGN < later)
            block_row = jnp.where(
                inside, jnp.where(into < ROWS, e * ROWS + into, n_local * ROWS + into - ROWS), block_row)
            start = later
        step_row = jnp.minimum(step_row, n_sorted)
        block_row = jnp.minimum(block_row, n_steps * ROWS - ALIGN)
        table_row = lax.broadcasted_iota(jnp.int32, (n_blocks, tokens), 0)
        sched_v[...] = jnp.where(
            table_row == 0, step_expert, jnp.where(table_row == 1, step_row // ALIGN, block_row // ALIGN))
        to_scalar = pltpu.make_async_copy(sched_v, sched, w_sem.at[8])
        to_scalar.start()

        place_s[...] = place
        weight_s[...] = weight
        row_id = lax.broadcasted_iota(jnp.int32, (n_sorted, tokens), 0)
        weight_rows = jnp.zeros((n_sorted, tokens), F32)
        spots = (chip, left, right, far)
        for n, spot in enumerate(spots):
            for c in range(2):
                source = pl.ds(c * n_x + spot, 1)
                match = row_id == place_s[source, :]
                first_col = (2 * n + c) * tokens
                sort[:, first_col:first_col + tokens] = jnp.where(match, 1.0, 0.0).astype(BF16)
                weight_rows = weight_rows + jnp.where(match, weight_s[source, :], 0.0)
        weight_sorted[0:n_sorted, :] = jnp.broadcast_to(
            jnp.sum(weight_rows, axis=1, keepdims=True), (n_sorted, 128))
        weight_sorted[n_sorted:, :] = jnp.zeros((ROWS, 128), F32)
        xs[n_sorted:, :] = jnp.zeros((ROWS, dim), BF16)
        place_cols = jnp.transpose(place.astype(F32))
        column_id = lax.broadcasted_iota(jnp.int32, (tokens, n_sorted), 1).astype(F32)
        for j in range(n_blocks):
            unsort[j * tokens:(j + 1) * tokens, :] = jnp.where(
                column_id == place_cols[:, j:j + 1], 1.0, 0.0).astype(BF16)

        forward(2, left, high)
        forward(4, right, low)
        attention_sum()

        def add_rows(numbers):
            def one(i, carry):
                cols = pl.ds(pl.multiple_of(i * 256, 256), 256)
                total = None
                for n in numbers:
                    rows = rows_all[:, spots[n], :, cols].reshape(2 * tokens, 256)
                    part = dot_nn(sort[:, 2 * n * tokens:(2 * n + 2) * tokens], rows)
                    total = part if total is None else total + part
                if numbers[0] > 0:
                    total = total + xs[0:n_sorted, cols].astype(F32)
                xs[0:n_sorted, cols] = total.astype(BF16)
                return carry

            lax.fori_loop(0, dim // 256, one, 0, unroll=2)

        arrived(rows_all.at[other, chip], ag_recv.at[0])
        for index, spot, part in ((1, left, low), (2, left, high), (3, right, high), (4, right, low)):
            arrived(rows_all.at[other, spot, part], ag_recv.at[index + 6])
        add_rows((0, 1, 2))
        forward(5, far, low)
        forward(6, far, high)
        for index, part in ((5, low), (6, high)):
            arrived(rows_all.at[other, far, part], ag_recv.at[index + 6])
        add_rows((3,))
        for index in range(1, 13):
            sent(rows_all.at[core, chip, low], ag_send.at[index])
        sent(rows_all.at[core, chip], ag_send.at[0])
        for k in range(1, n_ep):
            sent(meta.at[core * n_x + chip], m_send.at[k - 1])
            sent(all_ids.at[core * n_x + chip], i_send.at[k - 1])
        to_scalar.wait()
        for e in range(n_local):
            pltpu.make_async_copy(eg_hbm.at[e], eg.at[e], e_sem.at[0, e]).wait()
            pltpu.make_async_copy(eu_hbm.at[e], eu.at[e], e_sem.at[1, e]).wait()

        def gate_up(step, carry):
            e = sched[0, step]
            rows = xs[pl.ds(sched[1, step] * ALIGN, ROWS), :]
            act = jax.nn.silu(dot_nt(eg[e], rows)) * dot_nt(eu[e], rows)
            z[step] = jnp.transpose(act).astype(BF16)
            return carry

        lax.fori_loop(0, n_steps, gate_up, 0, unroll=3)

        for p in range(dense_parts):
            pltpu.make_async_copy(wg_hbm.at[p], eg.at[p], w_sem.at[p]).start()
            pltpu.make_async_copy(wu_hbm.at[p], eu.at[p], w_sem.at[2 + p]).start()
            pltpu.make_async_copy(wd_hbm.at[p], eg.at[dense_parts + p], w_sem.at[4 + p]).start()
        for e in range(n_local):
            pltpu.make_async_copy(ed_hbm.at[e], ed.at[e], e_sem.at[2, e]).wait()

        def compute(i):
            cols = columns(i)

            def down(step, carry):
                e = sched[0, step]
                scale = weight_sorted[pl.ds(sched[1, step] * ALIGN, ROWS), :]
                prod = dot_nn(z[step], ed[e, :, cols])
                scaled = [prod[:, b * 128:(b + 1) * 128] * scale for b in range(quarter // 128)]
                ys[pl.ds(pl.multiple_of(step * ROWS, ROWS), ROWS), :] = jnp.concatenate(scaled, axis=1).astype(BF16)
                return carry

            lax.fori_loop(0, n_steps, down, 0, unroll=3)

            def regroup(b, carry):
                y_sorted[pl.ds(pl.multiple_of(b * ALIGN, ALIGN), ALIGN), :] = ys[pl.ds(sched[2, b] * ALIGN, ALIGN), :]
                return carry

            lax.fori_loop(0, n_sorted // ALIGN, regroup, 0, unroll=8)
            for c in range(2):
                back = dot_nn(unsort[c * n_x * tokens:(c + 1) * n_x * tokens, :], y_sorted[...])
                rows_all[c, :, :, cols] = back.astype(BF16).reshape(n_x, tokens, quarter)
            remote(rows_all.at[other, :, :, cols], d_in.at[i], d_send.at[i], d_recv.at[i], partner).start()

        compute(0)
        dense_gate_up(act_s)
        pair_sum(0)
        compute(1)
        ring_sum(0)
        dense_down(act_s)
        pair_sum(1)
        compute(2)
        ring_sum(1)
        finish(0)
        pair_sum(2)
        compute(3)
        ring_sum(2)
        finish(1)
        pair_sum(3)
        ring_sum(3)
        finish(2)
        finish(3)

    def columns(i):
        return pl.ds(pl.multiple_of(((tp + 1 + i) % n_tp) * quarter, quarter), quarter)

    def pair_sum(i):
        cols = columns(i)
        arrived(d_in.at[i], d_recv.at[i])
        for spot in range(n_x):
            rows_all[core, spot, :, cols] = (
                rows_all[core, spot, :, cols].astype(F32) + d_in[i, spot].astype(F32)).astype(BF16)
        remote(rows_all.at[core, far, low, cols], r1_in.at[i, 0], r1_send.at[i, 0], r1_recv.at[i, 0], on_ring(right)).start()
        remote(rows_all.at[core, far, high, cols], r1_in.at[i, 1], r1_send.at[i, 1], r1_recv.at[i, 1], on_ring(left)).start()
        remote(rows_all.at[core, right, high, cols], r2_in.at[i, 0, high], r2_send.at[i, 0], r2_recv.at[i, 0], on_ring(right)).start()
        remote(rows_all.at[core, left, low, cols], r2_in.at[i, 1, low], r2_send.at[i, 1], r2_recv.at[i, 1], on_ring(left)).start()

    def ring_sum(i):
        cols = columns(i)
        arrived(r1_in.at[i, 0], r1_recv.at[i, 0])
        rows_all[core, right, low, cols] = (
            rows_all[core, right, low, cols].astype(F32) + r1_in[i, 0].astype(F32)).astype(BF16)
        remote(rows_all.at[core, right, low, cols], r2_in.at[i, 0, low], r2_send.at[i, 2], r2_recv.at[i, 2], on_ring(right)).start()
        arrived(r1_in.at[i, 1], r1_recv.at[i, 1])
        rows_all[core, left, high, cols] = (
            rows_all[core, left, high, cols].astype(F32) + r1_in[i, 1].astype(F32)).astype(BF16)
        remote(rows_all.at[core, left, high, cols], r2_in.at[i, 1, high], r2_send.at[i, 3], r2_recv.at[i, 3], on_ring(left)).start()

    def dense_gate_up(act_s):
        for k in range(1, n_tp):
            source = (tp + n_tp - k) % n_tp
            arrived(h_q.at[source], h_recv.at[k - 1])
        hidden_mid = jnp.concatenate([h_q[q] for q in range(n_tp)], axis=1)
        c_buf[...] = rms_norm(hidden_mid, as_row(n_res_ref[...]))
        for p in range(dense_parts):
            pltpu.make_async_copy(wg_hbm.at[p], eg.at[p], w_sem.at[p]).wait()
            pltpu.make_async_copy(wu_hbm.at[p], eu.at[p], w_sem.at[2 + p]).wait()
            act = jax.nn.silu(dot_nt(eg[p], c_buf[...])) * dot_nt(eu[p], c_buf[...])
            act_s[p] = jnp.transpose(act).astype(BF16)

    def dense_down(act_s):
        for p in range(dense_parts):
            pltpu.make_async_copy(wd_hbm.at[p], eg.at[dense_parts + p], w_sem.at[4 + p]).wait()
        for q in range(n_tp):
            cols = slice(q * quarter, (q + 1) * quarter)
            dense = dot_nn(act_s[0], eg[dense_parts, :, cols])
            for p in range(1, dense_parts):
                dense = dense + dot_nn(act_s[p], eg[dense_parts + p, :, cols])
            dense_q[q] = dense

    def finish(i):
        q = (tp + 1 + i) % n_tp
        cols = columns(i)
        arrived(r2_in.at[i, 0, high], r2_recv.at[i, 0])
        arrived(r2_in.at[i, 1, low], r2_recv.at[i, 1])
        arrived(r2_in.at[i, 0, low], r2_recv.at[i, 2])
        arrived(r2_in.at[i, 1, high], r2_recv.at[i, 3])
        part = rows_all[core, chip, :, cols].astype(F32) + r2_in[i, 0].astype(F32) + r2_in[i, 1].astype(F32) + dense_q[q]
        if i < n_tp - 1:
            fin_q[i] = part.astype(BF16)
            remote(fin_q.at[i], fin_in.at[i], f_send.at[i], f_recv.at[i], tp_peer(i + 1)).start()
        else:
            for k in range(1, n_tp):
                arrived(fin_in.at[k - 1], f_recv.at[k - 1])
                part = part + fin_in[k - 1].astype(F32)
            out_q[tp] = (h_q[tp].astype(F32) + part).astype(BF16)

    pl.run_scoped(
        expert_phase,
        pltpu.VMEM((n_sorted + ROWS, dim), BF16),
        pltpu.VMEM((n_sorted, all_rows), BF16),
        pltpu.VMEM((all_rows, n_sorted), BF16),
        pltpu.VMEM((n_steps, ROWS, width), BF16),
        pltpu.VMEM((n_steps * ROWS, quarter), BF16),
        pltpu.VMEM((n_sorted, quarter), BF16),
        pltpu.VMEM((n_sorted + ROWS, 128), F32),
        pltpu.VMEM((n_blocks, tokens), jnp.int32),
        pltpu.VMEM((n_blocks, tokens), F32),
        pltpu.VMEM((dense_parts, tokens, width), BF16),
    )
    for k in range(1, n_tp):
        remote(out_q.at[tp], out_q.at[tp], o_send.at[k - 1], o_recv.at[k - 1], tp_peer(k)).start()

    for i in range(n_tp):
        cols = columns(i)
        sent(d_in.at[i], d_send.at[i])
        for side in range(2):
            sent(r1_in.at[i, side], r1_send.at[i, side])
        for message in range(4):
            sent(r1_in.at[i, 0], r2_send.at[i, message])
    for k in range(1, n_tp):
        sent(part_in.at[k - 1], a_send.at[k - 1])
        sent(part_in.at[k - 1], h_send.at[k - 1])
        sent(part_in.at[k - 1], f_send.at[k - 1])
    for k in range(1, n_tp):
        source = (tp + n_tp - k) % n_tp
        arrived(out_q.at[source], o_recv.at[k - 1])
    for q in range(n_tp):
        out_ref[:, q * quarter:(q + 1) * quarter] = out_q[q]
    for k in range(1, n_tp):
        sent(part_in.at[k - 1], o_send.at[k - 1])


def cache_kernel(pieces, pos, hidden_ref, k_new, v_new, k_hbm, v_hbm, out_ref, k_out, v_out, k_buf, v_buf, in_sem, out_sem):
    size = k_buf.shape[0] // pieces
    both = ((k_hbm, k_buf, k_out, k_new), (v_hbm, v_buf, v_out, v_new))
    loads = [
        [pltpu.make_async_copy(src.at[pl.ds(i * size, size)], buf.at[pl.ds(i * size, size)], in_sem.at[n, i])
         for n, (src, buf, _, _) in enumerate(both)] for i in range(pieces)]
    stores = [
        [pltpu.make_async_copy(buf.at[pl.ds(i * size, size)], dst.at[pl.ds(i * size, size)], out_sem.at[n, i])
         for n, (_, buf, dst, _) in enumerate(both)] for i in range(pieces)]
    for pair in loads:
        for load in pair:
            load.start()
    out_ref[...] = hidden_ref[...]
    for i in range(pieces):
        for n, (_, buf, _, new) in enumerate(both):
            loads[i][n].wait()
            for t in range(i * size, (i + 1) * size):
                buf[t, pos[t]] = new[t]
            stores[i][n].start()
    for pair in stores:
        for store in pair:
            store.wait()


def rope_table(cache_len, head_dim):
    freq = 1.0 / (ROPE_BASE ** (np.arange(0, head_dim, 2, dtype=np.float32) / np.float32(head_dim)))
    angle = np.arange(cache_len, dtype=np.float32)[:, None] * freq.astype(np.float32)[None, :]
    cosine, sine = np.cos(angle), np.sin(angle)
    return np.concatenate(
        [np.concatenate([cosine, cosine], 1), np.concatenate([-sine, sine], 1)], 0).astype(np.float32)


def solution(mesh):
    n_tp, n_ep = mesh.shape['tp'], mesh.shape['ep']
    row_spec = P(('dp', 'ep'), None)
    cache_spec = P(('dp', 'ep'), None, 'tp', None)
    col_split = P(None, 'tp')
    row_split = P('tp', None)
    in_specs = (row_spec, P(('dp', 'ep')), row_spec, cache_spec, cache_spec, P(None), P(None), P(None), col_split, col_split, col_split, row_split, col_split, col_split, row_split, P(None, None), P('ep', None, 'tp'), P('ep', None, 'tp'), P('ep', 'tp', None))
    out_specs = (row_spec, cache_spec, cache_spec)

    def local_layer(hidden_in, positions, expert_ids, k_cache, v_cache, norm_in, norm_res, norm_post, w_q, w_k, w_v, w_o, w_gate, w_up, w_down, w_router, e_gate, e_up, e_down):
        tokens, dim = hidden_in.shape
        n_local, width = e_gate.shape[0], e_gate.shape[2]
        cache_len, heads, head_dim = k_cache.shape[1:]
        dense_parts = w_down.shape[0] // width
        quarter = dim // n_tp
        n_x = n_ep // 2
        half = tokens // 2
        vmem = pl.BlockSpec(memory_space=pltpu.VMEM)
        hbm = pl.BlockSpec(memory_space=pl.ANY)
        dma = pltpu.SemaphoreType.DMA
        hidden, k_new, v_new = pl.pallas_call(
            functools.partial(layer_kernel, n_tp, n_ep, 'ep', 'tp'),
            out_shape=(
                jax.ShapeDtypeStruct(hidden_in.shape, BF16),
                jax.ShapeDtypeStruct((tokens * heads, head_dim), BF16),
                jax.ShapeDtypeStruct((tokens * heads, head_dim), BF16),
            ),
            in_specs=[vmem] * 8 + [hbm] * 12,
            out_specs=(vmem, vmem, vmem),
            scratch_shapes=[
                pltpu.VMEM((n_local, width, dim), BF16),
                pltpu.VMEM((n_local, width, dim), BF16),
                pltpu.VMEM((n_local, width, dim), BF16),
                pltpu.VMEM((2, n_x, tokens, dim), BF16),
                pltpu.VMEM((n_ep, 8, tokens), F32),
                pltpu.VMEM((n_ep, 8, tokens), jnp.int32),
                pltpu.VMEM((n_tp, tokens, quarter), BF16),
                pltpu.VMEM((n_tp - 1, tokens, quarter), BF16),
                pltpu.VMEM((n_tp, tokens, quarter), BF16),
                pltpu.VMEM((tokens, dim), BF16),
                pltpu.VMEM((n_tp, n_x, tokens, quarter), BF16),
                pltpu.VMEM((n_tp, 2, half, quarter), BF16),
                pltpu.VMEM((n_tp, 2, tokens, quarter), BF16),
                pltpu.VMEM((n_tp, tokens, quarter), F32),
                pltpu.VMEM((n_tp - 1, tokens, quarter), BF16),
                pltpu.VMEM((n_tp - 1, tokens, quarter), BF16),
                pltpu.VMEM((n_tp, tokens, quarter), BF16),
                pltpu.VMEM((n_ep, tokens), jnp.int32),
                pltpu.SMEM((n_ep, tokens), jnp.int32),
                dma((9,)), dma((3, n_local)), dma((13,)), dma((13,)), *[dma((n_ep - 1,))] * 4,
                *[dma((n_tp - 1,))] * 4,
                dma((n_tp,)), dma((n_tp,)),
                dma((n_tp, 2)), dma((n_tp, 2)), dma((n_tp, 4)), dma((n_tp, 4)),
                *[dma((n_tp - 1,))] * 4,
            ],
            compiler_params=pltpu.CompilerParams(
                collective_id=0, has_side_effects=True, vmem_limit_bytes=67043328),
        )(
            hidden_in, positions.reshape(1, tokens), expert_ids.T,
            norm_in.reshape(-1, 128), norm_res.reshape(-1, 128), norm_post.reshape(-1, 128), w_router.T,
            jnp.asarray(rope_table(cache_len, head_dim)),
            k_cache.reshape(-1, head_dim), v_cache.reshape(-1, head_dim), w_q, w_k, w_v, w_o,
            w_gate.T.reshape(dense_parts, width, dim), w_up.T.reshape(dense_parts, width, dim),
            w_down.reshape(dense_parts, width, dim),
            jnp.swapaxes(e_gate, 1, 2), jnp.swapaxes(e_up, 1, 2), e_down,
        )
        return pl.pallas_call(
            functools.partial(cache_kernel, 8),
            out_shape=(
                jax.ShapeDtypeStruct(hidden_in.shape, BF16),
                jax.ShapeDtypeStruct(k_cache.shape, BF16),
                jax.ShapeDtypeStruct(v_cache.shape, BF16),
            ),
            in_specs=[pl.BlockSpec(memory_space=pltpu.SMEM), vmem, vmem, vmem, hbm, hbm],
            out_specs=(vmem, hbm, hbm),
            scratch_shapes=[
                pltpu.VMEM(k_cache.shape, BF16), pltpu.VMEM(v_cache.shape, BF16),
                dma((2, 8)), dma((2, 8)),
            ],
        )(positions, hidden, k_new.reshape(tokens, heads, head_dim), v_new.reshape(tokens, heads, head_dim), k_cache, v_cache)

    return jax.shard_map(local_layer, mesh=mesh, in_specs=in_specs, out_specs=out_specs, check_vma=False)
```

```python
import functools

import jax
import jax.numpy as jnp
import numpy as np
from jax import lax
from jax.experimental import pallas as pl
from jax.experimental.pallas import tpu as pltpu
from jax.sharding import PartitionSpec as P

NORM_EPS = 1e-5
ROPE_BASE = 10000.0
F32 = jnp.float32
BF16 = jnp.bfloat16
MESH = pl.DeviceIdType.MESH
ROWS = 256
ALIGN = 16


def as_row(gains):
    wide = gains.astype(F32)
    return jnp.concatenate([wide[i:i + 1, :] for i in range(wide.shape[0])], axis=1)


def rms_norm(values, gain_row):
    wide_vals = values.astype(F32)
    inv_rms = lax.rsqrt(jnp.mean(wide_vals * wide_vals, axis=-1, keepdims=True) + NORM_EPS)
    return (wide_vals * inv_rms * gain_row.astype(F32)).astype(BF16)


def dot_nn(a, b):
    return lax.dot_general(a, b, (((1,), (0,)), ((), ())), preferred_element_type=F32)


def dot_nt(a, b):
    return lax.dot_general(a, b, (((1,), (1,)), ((), ())), preferred_element_type=F32)


def lane_scan(values):
    lane = lax.broadcasted_iota(jnp.int32, values.shape, 1)
    step = 1
    while step < values.shape[1]:
        values = values + jnp.where(lane >= step, pltpu.roll(values, step, 1), 0)
        step *= 2
    return values


def row_scan(values):
    row = lax.broadcasted_iota(jnp.int32, values.shape, 0)
    step = 1
    while step < values.shape[0]:
        values = values + jnp.where(row >= step, pltpu.roll(values, step, 0), 0)
        step *= 2
    return values


def layer_kernel(
    n_tp, n_ep, ep_axis, tp_axis,
    x_ref, pos_row_ref, ids_ref, n_in_ref, n_res_ref, n_post_ref, w_router_ref, rope_ref,
    k_hbm, v_hbm, wq_hbm, wk_hbm, wv_hbm, wo_hbm, wg_hbm, wu_hbm, wd_hbm, eg_hbm, eu_hbm, ed_hbm,
    out_ref, k_new, v_new,
    eg, eu, ed, rows_all, meta, all_ids, part_q, part_in, h_q, c_buf, d_in, r1_in, r2_in, dense_q, fin_q, fin_in, out_q,
    sched_v, sched,
    w_sem, e_sem, ag_send, ag_recv, m_send, m_recv, i_send, i_recv, a_send, a_recv, h_send, h_recv, d_send, d_recv,
    r1_send, r1_recv, r2_send, r2_recv, f_send, f_recv, o_send, o_recv,
):
    tokens, dim = x_ref.shape
    quarter = dim // n_tp
    n_x = n_ep // 2
    half = tokens // 2
    n_local, width = eg.shape[0], eg.shape[1]
    head_dim = k_hbm.shape[1]
    heads = wq_hbm.shape[1] // head_dim
    cache_len = k_hbm.shape[0] // (tokens * heads)
    n_blocks = n_ep
    all_rows = n_blocks * tokens
    n_sorted = -(-(4 * tokens + n_local * (ALIGN - 1)) // 128) * 128
    n_steps = n_local + 1
    dense_parts = wd_hbm.shape[0]

    ep = lax.axis_index(ep_axis)
    tp = lax.axis_index(tp_axis)
    chip = ep // 2
    core = ep % 2
    other = 1 - core
    right = (chip + 1) % n_x
    left = (chip + n_x - 1) % n_x
    far = (chip + 2) % n_x

    def on_ring(place):
        return {ep_axis: place * 2 + core}

    partner = {ep_axis: chip * 2 + other}

    def ep_peer(k):
        return {ep_axis: (ep + k) % n_ep}

    def tp_peer(k):
        return {tp_axis: (tp + k) % n_tp}

    def remote(src, dst, send_sem, recv_sem, device):
        return pltpu.make_async_remote_copy(
            src_ref=src, dst_ref=dst, send_sem=send_sem, recv_sem=recv_sem, device_id=device, device_id_type=MESH)

    def arrived(dst, recv_sem):
        remote(dst, dst, recv_sem, recv_sem, partner).wait_recv()

    def sent(src, send_sem):
        remote(src, src, send_sem, send_sem, partner).wait_send()

    low, high = pl.ds(0, half), pl.ds(half, half)

    def forward(index, place, rows):
        block = rows_all.at[core, place, rows]
        arrived(block, ag_recv.at[index])
        remote(block, block, ag_send.at[index + 6], ag_recv.at[index + 6], partner).start()

    def forward_first():
        forward(1, left, low)
        block = rows_all.at[core, left, low]
        remote(block, block, ag_send.at[5], ag_recv.at[5], on_ring(right)).start()
        forward(3, right, high)
        block = rows_all.at[core, right, high]
        remote(block, block, ag_send.at[6], ag_recv.at[6], on_ring(left)).start()

    barrier = pltpu.get_barrier_semaphore()
    for k in range(1, n_ep):
        pl.semaphore_signal(barrier, inc=1, device_id=ep_peer(k), device_id_type=MESH)
    for k in range(1, n_tp):
        pl.semaphore_signal(barrier, inc=1, device_id=tp_peer(k), device_id_type=MESH)

    def attention_phase(wq, wk, wv, wo, kc, vc, q_s, k_s, v_s, o_s, pos_s):
        loads = [
            pltpu.make_async_copy(src, dst, w_sem.at[i])
            for i, (src, dst) in enumerate(
                ((wq_hbm, wq), (wk_hbm, wk), (wv_hbm, wv), (k_hbm, kc), (v_hbm, vc), (wo_hbm, wo)))
        ]
        for load in loads:
            load.start()

        moe_in = rms_norm(x_ref[...], as_row(n_post_ref[...]))
        rows_all[core, chip] = moe_in
        logits = dot_nt(w_router_ref[...], moe_in)
        shifted = jnp.exp(logits - jnp.max(logits, axis=0, keepdims=True))
        probs = shifted / jnp.sum(shifted, axis=0, keepdims=True)
        expert_row = lax.broadcasted_iota(jnp.int32, probs.shape, 0)
        ids = ids_ref[...]
        picked = [
            jnp.sum(jnp.where(expert_row == ids[k:k + 1, :], probs, 0.0), axis=0, keepdims=True) for k in range(2)
        ]
        total = picked[0] + picked[1]
        meta[core * n_x + chip] = jnp.concatenate(
            [picked[0] / total, picked[1] / total, jnp.zeros((6, tokens), F32)], axis=0)
        all_ids[core * n_x + chip] = jnp.concatenate([ids, jnp.zeros((6, tokens), jnp.int32)], axis=0)

        pl.semaphore_wait(barrier, n_ep - 1 + n_tp - 1)
        own = rows_all.at[core, chip]
        sends = [
            remote(own.at[low], own.at[low], ag_send.at[1], ag_recv.at[1], on_ring(right)),
            remote(own.at[high], own.at[high], ag_send.at[3], ag_recv.at[3], on_ring(left)),
            remote(own.at[high], own.at[high], ag_send.at[2], ag_recv.at[2], on_ring(right)),
            remote(own.at[low], own.at[low], ag_send.at[4], ag_recv.at[4], on_ring(left)),
            remote(own, own, ag_send.at[0], ag_recv.at[0], partner),
        ]
        for k in range(1, n_ep):
            block = meta.at[core * n_x + chip]
            sends.append(remote(block, block, m_send.at[k - 1], m_recv.at[k - 1], ep_peer(k)))
            block = all_ids.at[core * n_x + chip]
            sends.append(remote(block, block, i_send.at[k - 1], i_recv.at[k - 1], ep_peer(k)))
        for send in sends:
            send.start()

        normed = rms_norm(x_ref[...], as_row(n_in_ref[...]))
        pos_col = jnp.transpose(jnp.broadcast_to(pos_row_ref[...].astype(F32), (tokens, tokens)))
        cosine = jnp.zeros((tokens, head_dim), F32)
        sine = jnp.zeros((tokens, head_dim), F32)
        for p in range(cache_len):
            cosine = jnp.where(pos_col == float(p), rope_ref[p:p + 1, :], cosine)
            sine = jnp.where(pos_col == float(p), rope_ref[cache_len + p:cache_len + p + 1, :], sine)

        def rotated(values):
            return values * cosine + pltpu.roll(values, head_dim // 2, 1) * sine

        for head in range(heads):
            pos_s[pl.ds(head, tokens, stride=heads), :] = pos_col
        for load, weights, dest in ((loads[0], wq, q_s), (loads[1], wk, k_s), (loads[2], wv, v_s)):
            load.wait()
            proj = dot_nn(normed, weights[...])
            for head in range(heads):
                values = proj[:, head * head_dim:(head + 1) * head_dim]
                if dest is not v_s:
                    values = rotated(values)
                dest[pl.ds(head, tokens, stride=heads), :] = values.astype(BF16).astype(F32)
        k_new[...] = k_s[...].astype(BF16)
        v_new[...] = v_s[...].astype(BF16)

        for e in range(n_local):
            pltpu.make_async_copy(eg_hbm.at[e], eg.at[e], e_sem.at[0, e]).start()
            pltpu.make_async_copy(eu_hbm.at[e], eu.at[e], e_sem.at[1, e]).start()
            pltpu.make_async_copy(ed_hbm.at[e], ed.at[e], e_sem.at[2, e]).start()

        loads[3].wait()
        loads[4].wait()
        group = 16 // heads
        q_rows, slots = 16, group * cache_len * heads
        shape = (q_rows, slots)
        row, col = lax.broadcasted_iota(jnp.int32, shape, 0), lax.broadcasted_iota(jnp.int32, shape, 1)
        own_rows = jnp.logical_and(row // heads == col // (cache_len * heads), row % heads == col % heads)
        slot = jnp.where(own_rows, col // heads % cache_len, cache_len).astype(F32)

        batch = 8

        def attend(step, carry):
            rows = [pl.ds(pl.multiple_of((step * batch + g) * q_rows, q_rows), q_rows) for g in range(batch)]
            wide_rows = [pl.ds(pl.multiple_of((step * batch + g) * slots, slots), slots) for g in range(batch)]
            query = [q_s[r, :] for r in rows]
            at = [pos_s[r, :] for r in rows]
            scores = [dot_nt(q.astype(BF16), kc[w, :]) * (head_dim ** -0.5) for q, w in zip(query, wide_rows)]
            score_new = [
                jnp.sum(q * k_s[r, :], axis=1, keepdims=True) * (head_dim ** -0.5) for q, r in zip(query, rows)]
            scores = [
                jnp.where(slot < jnp.concatenate([p] * (slots // 128), axis=1), x, -jnp.inf) for x, p in zip(scores, at)]
            top = [jnp.maximum(jnp.max(x, axis=1, keepdims=True), n) for x, n in zip(scores, score_new)]
            weights = [jnp.exp(x - t) for x, t in zip(scores, top)]
            weight_new = [jnp.exp(n - t) for n, t in zip(score_new, top)]
            total = [jnp.sum(w, axis=1, keepdims=True) + n for w, n in zip(weights, weight_new)]
            weights = [(w / t).astype(BF16) for w, t in zip(weights, total)]
            weight_new = [(n / t).astype(BF16).astype(F32) for n, t in zip(weight_new, total)]
            mix = [dot_nn(w, vc[r, :]) for w, r in zip(weights, wide_rows)]
            mix = [m + n * v_s[r, :] for m, n, r in zip(mix, weight_new, rows)]
            for m, r in zip(mix, rows):
                o_s[r, :] = m
            return carry

        lax.fori_loop(0, tokens // group // batch, attend, 0)

        forward_first()

        mixed = jnp.concatenate(
            [o_s[pl.ds(head, tokens, stride=heads), :] for head in range(heads)], axis=1).astype(BF16)
        loads[5].wait()
        for q in range(n_tp):
            part_q[q] = dot_nn(mixed, wo[:, q * quarter:(q + 1) * quarter]).astype(BF16)
        for k in range(1, n_tp):
            send = remote(part_q.at[(tp + k) % n_tp], part_in.at[k - 1], a_send.at[k - 1], a_recv.at[k - 1], tp_peer(k))
            send.start()

    pl.run_scoped(
        attention_phase,
        *[pltpu.VMEM((dim, heads * head_dim), BF16)] * 3,
        pltpu.VMEM((heads * head_dim, dim), BF16),
        *[pltpu.VMEM(k_hbm.shape, BF16)] * 2,
        *[pltpu.VMEM((tokens * heads, head_dim), F32)] * 5,
    )

    def attention_sum():
        mine = pl.ds(pl.multiple_of(tp * quarter, quarter), quarter)
        for k in range(1, n_tp):
            arrived(part_in.at[k - 1], a_recv.at[k - 1])
        attn_sum = part_q[tp].astype(F32)
        for k in range(1, n_tp):
            attn_sum = attn_sum + part_in[k - 1].astype(F32)
        h_q[tp] = (x_ref[:, mine].astype(F32) + attn_sum).astype(BF16)
        for k in range(1, n_tp):
            remote(h_q.at[tp], h_q.at[tp], h_send.at[k - 1], h_recv.at[k - 1], tp_peer(k)).start()

    def expert_phase(xs, sort, unsort, z, ys, y_sorted, weight_sorted, place_s, weight_s, act_s):
        for k in range(1, n_ep):
            source = (ep + n_ep - k) % n_ep
            arrived(meta.at[(source % 2) * n_x + source // 2], m_recv.at[k - 1])
            arrived(all_ids.at[(source % 2) * n_x + source // 2], i_recv.at[k - 1])
        ids = [all_ids[:, k, :] for k in range(2)]
        wts = [meta[:, k, :] for k in range(2)]
        first = ep * n_local
        lane = lax.broadcasted_iota(jnp.int32, (n_blocks, tokens), 1)
        start = jnp.zeros((n_blocks, tokens), jnp.int32)
        place = jnp.full((n_blocks, tokens), -1, jnp.int32)
        weight = jnp.zeros((n_blocks, tokens), F32)
        step_expert = jnp.zeros((n_blocks, tokens), jnp.int32)
        step_row = jnp.zeros((n_blocks, tokens), jnp.int32)
        block_row = jnp.zeros((n_blocks, tokens), jnp.int32)
        for e in range(n_local):
            here = [i == first + e for i in ids]
            hit = jnp.where(jnp.logical_or(here[0], here[1]), 1, 0)
            weight = jnp.where(here[0], wts[0], jnp.where(here[1], wts[1], weight))
            scan = lane_scan(hit)
            totals = jnp.broadcast_to(scan[:, tokens - 1:], scan.shape)
            above = row_scan(totals)
            count = jnp.broadcast_to(above[n_blocks - 1:, :], scan.shape)
            place = jnp.where(hit == 1, start + above - totals + scan - 1, place)
            step_row = jnp.where(lane == e, start, step_row)
            step_expert = jnp.where(lane == e, e, step_expert)
            spill = jnp.logical_and(lane == n_local, count > ROWS)
            step_row = jnp.where(spill, start + ROWS, step_row)
            step_expert = jnp.where(spill, e, step_expert)
            later = start + (count + ALIGN - 1) // ALIGN * ALIGN
            into = lane * ALIGN - start
            inside = jnp.logical_and(into >= 0, lane * ALIGN < later)
            block_row = jnp.where(
                inside, jnp.where(into < ROWS, e * ROWS + into, n_local * ROWS + into - ROWS), block_row)
            start = later
        step_row = jnp.minimum(step_row, n_sorted)
        block_row = jnp.minimum(block_row, n_steps * ROWS - ALIGN)
        table_row = lax.broadcasted_iota(jnp.int32, (n_blocks, tokens), 0)
        sched_v[...] = jnp.where(
            table_row == 0, step_expert, jnp.where(table_row == 1, step_row // ALIGN, block_row // ALIGN))
        to_scalar = pltpu.make_async_copy(sched_v, sched, w_sem.at[8])
        to_scalar.start()

        place_s[...] = place
        weight_s[...] = weight
        row_id = lax.broadcasted_iota(jnp.int32, (n_sorted, tokens), 0)
        weight_rows = jnp.zeros((n_sorted, tokens), F32)
        spots = (chip, left, right, far)
        for n, spot in enumerate(spots):
            for c in range(2):
                source = pl.ds(c * n_x + spot, 1)
                match = row_id == place_s[source, :]
                first_col = (2 * n + c) * tokens
                sort[:, first_col:first_col + tokens] = jnp.where(match, 1.0, 0.0).astype(BF16)
                weight_rows = weight_rows + jnp.where(match, weight_s[source, :], 0.0)
        weight_sorted[0:n_sorted, :] = jnp.broadcast_to(
            jnp.sum(weight_rows, axis=1, keepdims=True), (n_sorted, 128))
        weight_sorted[n_sorted:, :] = jnp.zeros((ROWS, 128), F32)
        xs[n_sorted:, :] = jnp.zeros((ROWS, dim), BF16)
        place_cols = jnp.transpose(place.astype(F32))
        column_id = lax.broadcasted_iota(jnp.int32, (tokens, n_sorted), 1).astype(F32)
        for j in range(n_blocks):
            unsort[j * tokens:(j + 1) * tokens, :] = jnp.where(
                column_id == place_cols[:, j:j + 1], 1.0, 0.0).astype(BF16)

        forward(2, left, high)
        forward(4, right, low)
        attention_sum()

        def add_rows(numbers):
            def one(i, carry):
                cols = pl.ds(pl.multiple_of(i * 256, 256), 256)
                total = None
                for n in numbers:
                    rows = rows_all[:, spots[n], :, cols].reshape(2 * tokens, 256)
                    part = dot_nn(sort[:, 2 * n * tokens:(2 * n + 2) * tokens], rows)
                    total = part if total is None else total + part
                if numbers[0] > 0:
                    total = total + xs[0:n_sorted, cols].astype(F32)
                xs[0:n_sorted, cols] = total.astype(BF16)
                return carry

            lax.fori_loop(0, dim // 256, one, 0, unroll=2)

        arrived(rows_all.at[other, chip], ag_recv.at[0])
        for index, spot, part in ((1, left, low), (2, left, high), (3, right, high), (4, right, low)):
            arrived(rows_all.at[other, spot, part], ag_recv.at[index + 6])
        add_rows((0, 1, 2))
        forward(5, far, low)
        forward(6, far, high)
        for index, part in ((5, low), (6, high)):
            arrived(rows_all.at[other, far, part], ag_recv.at[index + 6])
        add_rows((3,))
        for index in range(1, 13):
            sent(rows_all.at[core, chip, low], ag_send.at[index])
        sent(rows_all.at[core, chip], ag_send.at[0])
        for k in range(1, n_ep):
            sent(meta.at[core * n_x + chip], m_send.at[k - 1])
            sent(all_ids.at[core * n_x + chip], i_send.at[k - 1])
        to_scalar.wait()
        for e in range(n_local):
            pltpu.make_async_copy(eg_hbm.at[e], eg.at[e], e_sem.at[0, e]).wait()
            pltpu.make_async_copy(eu_hbm.at[e], eu.at[e], e_sem.at[1, e]).wait()

        def gate_up(step, carry):
            e = sched[0, step]
            rows = xs[pl.ds(sched[1, step] * ALIGN, ROWS), :]
            act = jax.nn.silu(dot_nt(eg[e], rows)) * dot_nt(eu[e], rows)
            z[step] = jnp.transpose(act).astype(BF16)
            return carry

        lax.fori_loop(0, n_steps, gate_up, 0, unroll=3)

        for p in range(dense_parts):
            pltpu.make_async_copy(wg_hbm.at[p], eg.at[p], w_sem.at[p]).start()
            pltpu.make_async_copy(wu_hbm.at[p], eu.at[p], w_sem.at[2 + p]).start()
            pltpu.make_async_copy(wd_hbm.at[p], eg.at[dense_parts + p], w_sem.at[4 + p]).start()
        for e in range(n_local):
            pltpu.make_async_copy(ed_hbm.at[e], ed.at[e], e_sem.at[2, e]).wait()

        def compute(i):
            cols = columns(i)

            def down(step, carry):
                e = sched[0, step]
                scale = weight_sorted[pl.ds(sched[1, step] * ALIGN, ROWS), :]
                prod = dot_nn(z[step], ed[e, :, cols])
                scaled = [prod[:, b * 128:(b + 1) * 128] * scale for b in range(quarter // 128)]
                ys[pl.ds(pl.multiple_of(step * ROWS, ROWS), ROWS), :] = jnp.concatenate(scaled, axis=1).astype(BF16)
                return carry

            lax.fori_loop(0, n_steps, down, 0, unroll=3)

            def regroup(b, carry):
                y_sorted[pl.ds(pl.multiple_of(b * ALIGN, ALIGN), ALIGN), :] = ys[pl.ds(sched[2, b] * ALIGN, ALIGN), :]
                return carry

            lax.fori_loop(0, n_sorted // ALIGN, regroup, 0, unroll=8)
            for c in range(2):
                back = dot_nn(unsort[c * n_x * tokens:(c + 1) * n_x * tokens, :], y_sorted[...])
                rows_all[c, :, :, cols] = back.astype(BF16).reshape(n_x, tokens, quarter)
            remote(rows_all.at[other, :, :, cols], d_in.at[i], d_send.at[i], d_recv.at[i], partner).start()

        compute(0)
        dense_gate_up(act_s)
        pair_sum(0)
        compute(1)
        ring_sum(0)
        dense_down(act_s)
        pair_sum(1)
        compute(2)
        ring_sum(1)
        finish(0)
        pair_sum(2)
        compute(3)
        ring_sum(2)
        finish(1)
        pair_sum(3)
        ring_sum(3)
        finish(2)
        finish(3)

    def columns(i):
        return pl.ds(pl.multiple_of(((tp + 1 + i) % n_tp) * quarter, quarter), quarter)

    def pair_sum(i):
        cols = columns(i)
        arrived(d_in.at[i], d_recv.at[i])
        for spot in range(n_x):
            rows_all[core, spot, :, cols] = (
                rows_all[core, spot, :, cols].astype(F32) + d_in[i, spot].astype(F32)).astype(BF16)
        remote(rows_all.at[core, far, low, cols], r1_in.at[i, 0], r1_send.at[i, 0], r1_recv.at[i, 0], on_ring(right)).start()
        remote(rows_all.at[core, far, high, cols], r1_in.at[i, 1], r1_send.at[i, 1], r1_recv.at[i, 1], on_ring(left)).start()
        remote(rows_all.at[core, right, high, cols], r2_in.at[i, 0, high], r2_send.at[i, 0], r2_recv.at[i, 0], on_ring(right)).start()
        remote(rows_all.at[core, left, low, cols], r2_in.at[i, 1, low], r2_send.at[i, 1], r2_recv.at[i, 1], on_ring(left)).start()

    def ring_sum(i):
        cols = columns(i)
        arrived(r1_in.at[i, 0], r1_recv.at[i, 0])
        rows_all[core, right, low, cols] = (
            rows_all[core, right, low, cols].astype(F32) + r1_in[i, 0].astype(F32)).astype(BF16)
        remote(rows_all.at[core, right, low, cols], r2_in.at[i, 0, low], r2_send.at[i, 2], r2_recv.at[i, 2], on_ring(right)).start()
        arrived(r1_in.at[i, 1], r1_recv.at[i, 1])
        rows_all[core, left, high, cols] = (
            rows_all[core, left, high, cols].astype(F32) + r1_in[i, 1].astype(F32)).astype(BF16)
        remote(rows_all.at[core, left, high, cols], r2_in.at[i, 1, high], r2_send.at[i, 3], r2_recv.at[i, 3], on_ring(left)).start()

    def dense_gate_up(act_s):
        for k in range(1, n_tp):
            source = (tp + n_tp - k) % n_tp
            arrived(h_q.at[source], h_recv.at[k - 1])
        hidden_mid = jnp.concatenate([h_q[q] for q in range(n_tp)], axis=1)
        c_buf[...] = rms_norm(hidden_mid, as_row(n_res_ref[...]))
        for p in range(dense_parts):
            pltpu.make_async_copy(wg_hbm.at[p], eg.at[p], w_sem.at[p]).wait()
            pltpu.make_async_copy(wu_hbm.at[p], eu.at[p], w_sem.at[2 + p]).wait()
            act = jax.nn.silu(dot_nt(eg[p], c_buf[...])) * dot_nt(eu[p], c_buf[...])
            act_s[p] = jnp.transpose(act).astype(BF16)

    def dense_down(act_s):
        for p in range(dense_parts):
            pltpu.make_async_copy(wd_hbm.at[p], eg.at[dense_parts + p], w_sem.at[4 + p]).wait()
        for q in range(n_tp):
            cols = slice(q * quarter, (q + 1) * quarter)
            dense = dot_nn(act_s[0], eg[dense_parts, :, cols])
            for p in range(1, dense_parts):
                dense = dense + dot_nn(act_s[p], eg[dense_parts + p, :, cols])
            dense_q[q] = dense

    def finish(i):
        q = (tp + 1 + i) % n_tp
        cols = columns(i)
        arrived(r2_in.at[i, 0, high], r2_recv.at[i, 0])
        arrived(r2_in.at[i, 1, low], r2_recv.at[i, 1])
        arrived(r2_in.at[i, 0, low], r2_recv.at[i, 2])
        arrived(r2_in.at[i, 1, high], r2_recv.at[i, 3])
        part = rows_all[core, chip, :, cols].astype(F32) + r2_in[i, 0].astype(F32) + r2_in[i, 1].astype(F32) + dense_q[q]
        if i < n_tp - 1:
            fin_q[i] = part.astype(BF16)
            remote(fin_q.at[i], fin_in.at[i], f_send.at[i], f_recv.at[i], tp_peer(i + 1)).start()
        else:
            for k in range(1, n_tp):
                arrived(fin_in.at[k - 1], f_recv.at[k - 1])
                part = part + fin_in[k - 1].astype(F32)
            out_q[tp] = (h_q[tp].astype(F32) + part).astype(BF16)

    pl.run_scoped(
        expert_phase,
        pltpu.VMEM((n_sorted + ROWS, dim), BF16),
        pltpu.VMEM((n_sorted, all_rows), BF16),
        pltpu.VMEM((all_rows, n_sorted), BF16),
        pltpu.VMEM((n_steps, ROWS, width), BF16),
        pltpu.VMEM((n_steps * ROWS, quarter), BF16),
        pltpu.VMEM((n_sorted, quarter), BF16),
        pltpu.VMEM((n_sorted + ROWS, 128), F32),
        pltpu.VMEM((n_blocks, tokens), jnp.int32),
        pltpu.VMEM((n_blocks, tokens), F32),
        pltpu.VMEM((dense_parts, tokens, width), BF16),
    )
    before, after, across = (tp + n_tp - 1) % n_tp, (tp + 1) % n_tp, (tp + 2) % n_tp
    up, down = tp_peer(1), tp_peer(n_tp - 1)

    def pass_on(index, place, rows, device):
        block = out_q.at[place, rows]
        remote(block, block, o_send.at[index], o_recv.at[index], device).start()

    pass_on(0, tp, low, up)
    pass_on(1, tp, high, down)
    pass_on(2, tp, high, up)
    pass_on(3, tp, low, down)
    arrived(out_q.at[before, low], o_recv.at[0])
    pass_on(4, before, low, up)
    arrived(out_q.at[after, high], o_recv.at[1])
    pass_on(5, after, high, down)

    for i in range(n_tp):
        cols = columns(i)
        sent(d_in.at[i], d_send.at[i])
        for side in range(2):
            sent(r1_in.at[i, side], r1_send.at[i, side])
        for message in range(4):
            sent(r1_in.at[i, 0], r2_send.at[i, message])
    for k in range(1, n_tp):
        sent(part_in.at[k - 1], a_send.at[k - 1])
        sent(part_in.at[k - 1], h_send.at[k - 1])
        sent(part_in.at[k - 1], f_send.at[k - 1])
    out_ref[:, pl.ds(pl.multiple_of(tp * quarter, quarter), quarter)] = out_q[tp]
    arrived(out_q.at[before, high], o_recv.at[2])
    arrived(out_q.at[after, low], o_recv.at[3])
    for place in (before, after):
        out_ref[:, pl.ds(pl.multiple_of(place * quarter, quarter), quarter)] = out_q[place]
    arrived(out_q.at[across, low], o_recv.at[4])
    arrived(out_q.at[across, high], o_recv.at[5])
    out_ref[:, pl.ds(pl.multiple_of(across * quarter, quarter), quarter)] = out_q[across]
    for index in range(6):
        sent(out_q.at[tp, low], o_send.at[index])


def cache_kernel(pieces, pos, hidden, k_new_hbm, v_new_hbm, k_hbm, v_hbm, out, k_out, v_out, hidden_buf, k_new, v_new, k_buf, v_buf, in_sem, out_sem, sem):
    size = k_buf.shape[0] // pieces
    both = ((k_hbm, k_buf, k_out, k_new), (v_hbm, v_buf, v_out, v_new))
    first = [
        pltpu.make_async_copy(k_new_hbm, k_new, sem.at[0]),
        pltpu.make_async_copy(v_new_hbm, v_new, sem.at[1]),
    ]
    hidden_in, hidden_out = (
        pltpu.make_async_copy(hidden, hidden_buf, sem.at[2]), pltpu.make_async_copy(hidden_buf, out, sem.at[3]))
    loads = [
        [pltpu.make_async_copy(src.at[pl.ds(i * size, size)], buf.at[pl.ds(i * size, size)], in_sem.at[n, i])
         for n, (src, buf, _, _) in enumerate(both)] for i in range(pieces)]
    stores = [
        [pltpu.make_async_copy(buf.at[pl.ds(i * size, size)], dst.at[pl.ds(i * size, size)], out_sem.at[n, i])
         for n, (_, buf, dst, _) in enumerate(both)] for i in range(pieces)]
    for load in first:
        load.start()
    for pair in loads:
        for load in pair:
            load.start()
    hidden_in.start()
    for load in first:
        load.wait()
    for i in range(pieces):
        for n, (_, buf, _, new) in enumerate(both):
            loads[i][n].wait()
            for t in range(i * size, (i + 1) * size):
                buf[t, pos[t]] = new[t]
            stores[i][n].start()
    hidden_in.wait()
    hidden_out.start()
    for pair in stores:
        for store in pair:
            store.wait()
    hidden_out.wait()


def rope_table(cache_len, head_dim):
    freq = 1.0 / (ROPE_BASE ** (np.arange(0, head_dim, 2, dtype=np.float32) / np.float32(head_dim)))
    angle = np.arange(cache_len, dtype=np.float32)[:, None] * freq.astype(np.float32)[None, :]
    cosine, sine = np.cos(angle), np.sin(angle)
    return np.concatenate(
        [np.concatenate([cosine, cosine], 1), np.concatenate([-sine, sine], 1)], 0).astype(np.float32)


def solution(mesh):
    n_tp, n_ep = mesh.shape['tp'], mesh.shape['ep']
    row_spec = P(('dp', 'ep'), None)
    cache_spec = P(('dp', 'ep'), None, 'tp', None)
    col_split = P(None, 'tp')
    row_split = P('tp', None)
    in_specs = (row_spec, P(('dp', 'ep')), row_spec, cache_spec, cache_spec, P(None), P(None), P(None), col_split, col_split, col_split, row_split, col_split, col_split, row_split, P(None, None), P('ep', None, 'tp'), P('ep', None, 'tp'), P('ep', 'tp', None))
    out_specs = (row_spec, cache_spec, cache_spec)

    def local_layer(hidden_in, positions, expert_ids, k_cache, v_cache, norm_in, norm_res, norm_post, w_q, w_k, w_v, w_o, w_gate, w_up, w_down, w_router, e_gate, e_up, e_down):
        tokens, dim = hidden_in.shape
        n_local, width = e_gate.shape[0], e_gate.shape[2]
        cache_len, heads, head_dim = k_cache.shape[1:]
        dense_parts = w_down.shape[0] // width
        quarter = dim // n_tp
        n_x = n_ep // 2
        half = tokens // 2
        vmem = pl.BlockSpec(memory_space=pltpu.VMEM)
        hbm = pl.BlockSpec(memory_space=pl.ANY)
        dma = pltpu.SemaphoreType.DMA
        hidden, k_new, v_new = pl.pallas_call(
            functools.partial(layer_kernel, n_tp, n_ep, 'ep', 'tp'),
            out_shape=(
                jax.ShapeDtypeStruct(hidden_in.shape, BF16),
                jax.ShapeDtypeStruct((tokens * heads, head_dim), BF16),
                jax.ShapeDtypeStruct((tokens * heads, head_dim), BF16),
            ),
            in_specs=[vmem] * 8 + [hbm] * 12,
            out_specs=(vmem, vmem, vmem),
            scratch_shapes=[
                pltpu.VMEM((n_local, width, dim), BF16),
                pltpu.VMEM((n_local, width, dim), BF16),
                pltpu.VMEM((n_local, width, dim), BF16),
                pltpu.VMEM((2, n_x, tokens, dim), BF16),
                pltpu.VMEM((n_ep, 8, tokens), F32),
                pltpu.VMEM((n_ep, 8, tokens), jnp.int32),
                pltpu.VMEM((n_tp, tokens, quarter), BF16),
                pltpu.VMEM((n_tp - 1, tokens, quarter), BF16),
                pltpu.VMEM((n_tp, tokens, quarter), BF16),
                pltpu.VMEM((tokens, dim), BF16),
                pltpu.VMEM((n_tp, n_x, tokens, quarter), BF16),
                pltpu.VMEM((n_tp, 2, half, quarter), BF16),
                pltpu.VMEM((n_tp, 2, tokens, quarter), BF16),
                pltpu.VMEM((n_tp, tokens, quarter), F32),
                pltpu.VMEM((n_tp - 1, tokens, quarter), BF16),
                pltpu.VMEM((n_tp - 1, tokens, quarter), BF16),
                pltpu.VMEM((n_tp, tokens, quarter), BF16),
                pltpu.VMEM((n_ep, tokens), jnp.int32),
                pltpu.SMEM((n_ep, tokens), jnp.int32),
                dma((9,)), dma((3, n_local)), dma((13,)), dma((13,)), *[dma((n_ep - 1,))] * 4,
                *[dma((n_tp - 1,))] * 4,
                dma((n_tp,)), dma((n_tp,)),
                dma((n_tp, 2)), dma((n_tp, 2)), dma((n_tp, 4)), dma((n_tp, 4)),
                *[dma((n_tp - 1,))] * 2, dma((6,)), dma((6,)),
            ],
            compiler_params=pltpu.CompilerParams(
                collective_id=0, has_side_effects=True, vmem_limit_bytes=67043328),
        )(
            hidden_in, positions.reshape(1, tokens), expert_ids.T,
            norm_in.reshape(-1, 128), norm_res.reshape(-1, 128), norm_post.reshape(-1, 128), w_router.T,
            jnp.asarray(rope_table(cache_len, head_dim)),
            k_cache.reshape(-1, head_dim), v_cache.reshape(-1, head_dim), w_q, w_k, w_v, w_o,
            w_gate.T.reshape(dense_parts, width, dim), w_up.T.reshape(dense_parts, width, dim),
            w_down.reshape(dense_parts, width, dim),
            jnp.swapaxes(e_gate, 1, 2), jnp.swapaxes(e_up, 1, 2), e_down,
        )
        return pl.pallas_call(
            functools.partial(cache_kernel, 8),
            out_shape=(
                jax.ShapeDtypeStruct(hidden_in.shape, BF16),
                jax.ShapeDtypeStruct(k_cache.shape, BF16),
                jax.ShapeDtypeStruct(v_cache.shape, BF16),
            ),
            in_specs=[pl.BlockSpec(memory_space=pltpu.SMEM)] + [hbm] * 5,
            out_specs=(hbm, hbm, hbm),
            scratch_shapes=[
                pltpu.VMEM(hidden_in.shape, BF16),
                pltpu.VMEM((tokens, heads, head_dim), BF16), pltpu.VMEM((tokens, heads, head_dim), BF16),
                pltpu.VMEM(k_cache.shape, BF16), pltpu.VMEM(v_cache.shape, BF16),
                dma((2, 8)), dma((2, 8)), dma((4,)),
            ],
        )(positions, hidden, k_new.reshape(tokens, heads, head_dim), v_new.reshape(tokens, heads, head_dim), k_cache, v_cache)

    return jax.shard_map(local_layer, mesh=mesh, in_specs=in_specs, out_specs=out_specs, check_vma=False)
```

```python
import functools

import jax
import jax.numpy as jnp
import numpy as np
from jax import lax
from jax.experimental import pallas as pl
from jax.experimental.pallas import tpu as pltpu
from jax.sharding import PartitionSpec as P

NORM_EPS = 1e-5
ROPE_BASE = 10000.0
F32 = jnp.float32
BF16 = jnp.bfloat16
MESH = pl.DeviceIdType.MESH
ROWS = 256
ALIGN = 16


def as_row(gains):
    wide = gains.astype(F32)
    return jnp.concatenate([wide[i:i + 1, :] for i in range(wide.shape[0])], axis=1)


def rms_norm(values, gain_row):
    wide_vals = values.astype(F32)
    inv_rms = lax.rsqrt(jnp.mean(wide_vals * wide_vals, axis=-1, keepdims=True) + NORM_EPS)
    return (wide_vals * inv_rms * gain_row.astype(F32)).astype(BF16)


def dot_nn(a, b):
    return lax.dot_general(a, b, (((1,), (0,)), ((), ())), preferred_element_type=F32)


def dot_nt(a, b):
    return lax.dot_general(a, b, (((1,), (1,)), ((), ())), preferred_element_type=F32)


def lane_scan(values):
    lane = lax.broadcasted_iota(jnp.int32, values.shape, 1)
    step = 1
    while step < values.shape[1]:
        values = values + jnp.where(lane >= step, pltpu.roll(values, step, 1), 0)
        step *= 2
    return values


def row_scan(values):
    row = lax.broadcasted_iota(jnp.int32, values.shape, 0)
    step = 1
    while step < values.shape[0]:
        values = values + jnp.where(row >= step, pltpu.roll(values, step, 0), 0)
        step *= 2
    return values


def layer_kernel(
    n_tp, n_ep, ep_axis, tp_axis,
    x_ref, pos_row_ref, ids_ref, n_in_ref, n_res_ref, n_post_ref, w_router_ref, rope_ref,
    k_hbm, v_hbm, wq_hbm, wk_hbm, wv_hbm, wo_hbm, wg_hbm, wu_hbm, wd_hbm, eg_hbm, eu_hbm, ed_hbm,
    out_ref, k_new, v_new,
    eg, eu, ed, rows_all, meta, all_ids, part_q, part_in, h_q, c_buf, d_in, r1_in, r2_in, dense_q, fin_q, fin_in, out_q,
    sched_v, sched,
    w_sem, e_sem, ag_send, ag_recv, m_send, m_recv, i_send, i_recv, y_send, y_recv, a_send, a_recv, h_send, h_recv, d_send, d_recv,
    r1_send, r1_recv, r2_send, r2_recv, f_send, f_recv, o_send, o_recv,
):
    tokens, dim = x_ref.shape
    quarter = dim // n_tp
    n_x = n_ep // 2
    half = tokens // 2
    n_local, width = eg.shape[0], eg.shape[1]
    head_dim = k_hbm.shape[1]
    heads = wq_hbm.shape[1] // head_dim
    cache_len = k_hbm.shape[0] // (tokens * heads)
    n_blocks = n_ep
    all_rows = n_blocks * tokens
    n_sorted = -(-(4 * tokens + n_local * (ALIGN - 1)) // 128) * 128
    n_steps = n_local + 1
    dense_parts = wd_hbm.shape[0]

    ep = lax.axis_index(ep_axis)
    tp = lax.axis_index(tp_axis)
    chip = ep // 2
    core = ep % 2
    other = 1 - core
    right = (chip + 1) % n_x
    left = (chip + n_x - 1) % n_x
    far = (chip + 2) % n_x

    def on_ring(place):
        return {ep_axis: place * 2 + core}

    partner = {ep_axis: chip * 2 + other}

    def ep_peer(k):
        return {ep_axis: (ep + k) % n_ep}

    def tp_peer(k):
        return {tp_axis: (tp + k) % n_tp}

    def remote(src, dst, send_sem, recv_sem, device):
        return pltpu.make_async_remote_copy(
            src_ref=src, dst_ref=dst, send_sem=send_sem, recv_sem=recv_sem, device_id=device, device_id_type=MESH)

    def arrived(dst, recv_sem):
        remote(dst, dst, recv_sem, recv_sem, partner).wait_recv()

    def sent(src, send_sem):
        remote(src, src, send_sem, send_sem, partner).wait_send()

    low, high = pl.ds(0, half), pl.ds(half, half)

    messages = {1: (left, low), 2: (left, high), 3: (right, high), 4: (right, low), 5: (far, low), 6: (far, high)}
    side = pl.ds(pl.multiple_of((tp % 2) * (dim // 2), dim // 2), dim // 2)
    side_in = pl.ds(pl.multiple_of((1 - tp % 2) * (dim // 2), dim // 2), dim // 2)

    def along_x(index):
        place = {5: left, 6: right}.get(index, chip)
        rows = messages[index][1]
        block = rows_all.at[core, place, rows, side]
        device = on_ring(right if index in (1, 2, 5) else left)
        remote(block, block, ag_send.at[index], ag_recv.at[index], device).start()

    def along_y(index):
        place, rows = messages[index]
        block = rows_all.at[core, place, rows, side]
        arrived(block, ag_recv.at[index])
        device = tp_peer(1) if rows is low else tp_peer(n_tp - 1)
        remote(block, block, y_send.at[index - 1], y_recv.at[index - 1], device).start()

    def across(index):
        place, rows = messages[index]
        arrived(rows_all.at[core, place, rows, side_in], y_recv.at[index - 1])
        block = rows_all.at[core, place, rows]
        remote(block, block, ag_send.at[index + 6], ag_recv.at[index + 6], partner).start()

    def arrived_across(index):
        place, rows = messages[index]
        arrived(rows_all.at[other, place, rows], ag_recv.at[index + 6])

    barrier = pltpu.get_barrier_semaphore()
    for k in range(1, n_ep):
        pl.semaphore_signal(barrier, inc=1, device_id=ep_peer(k), device_id_type=MESH)
    for k in range(1, n_tp):
        pl.semaphore_signal(barrier, inc=1, device_id=tp_peer(k), device_id_type=MESH)

    def attention_phase(wq, wk, wv, wo, kc, vc, q_s, k_s, v_s, o_s, pos_s):
        loads = [
            pltpu.make_async_copy(src, dst, w_sem.at[i])
            for i, (src, dst) in enumerate(
                ((wq_hbm, wq), (wk_hbm, wk), (wv_hbm, wv), (k_hbm, kc), (v_hbm, vc), (wo_hbm, wo)))
        ]
        loads[0].start()

        ids = ids_ref[...]
        all_ids[core * n_x + chip] = jnp.concatenate([ids, jnp.zeros((6, tokens), jnp.int32)], axis=0)
        pl.semaphore_wait(barrier, n_ep - 1 + n_tp - 1)
        for k in range(1, n_ep):
            block = all_ids.at[core * n_x + chip]
            remote(block, block, i_send.at[k - 1], i_recv.at[k - 1], ep_peer(k)).start()

        loads[1].start()
        loads[2].start()

        moe_in = rms_norm(x_ref[...], as_row(n_post_ref[...]))
        rows_all[core, chip] = moe_in
        along_x(1)
        along_x(3)
        own = rows_all.at[core, chip]
        remote(own, own, ag_send.at[0], ag_recv.at[0], partner).start()
        logits = dot_nt(w_router_ref[...], moe_in)
        shifted = jnp.exp(logits - jnp.max(logits, axis=0, keepdims=True))
        probs = shifted / jnp.sum(shifted, axis=0, keepdims=True)
        expert_row = lax.broadcasted_iota(jnp.int32, probs.shape, 0)
        picked = [
            jnp.sum(jnp.where(expert_row == ids[k:k + 1, :], probs, 0.0), axis=0, keepdims=True) for k in range(2)
        ]
        total = picked[0] + picked[1]
        meta[core * n_x + chip] = jnp.concatenate(
            [picked[0] / total, picked[1] / total, jnp.zeros((6, tokens), F32)], axis=0)

        def second_sends():
            along_x(2)
            along_x(4)
            for k in range(1, n_ep):
                block = meta.at[core * n_x + chip]
                remote(block, block, m_send.at[k - 1], m_recv.at[k - 1], ep_peer(k)).start()

        normed = rms_norm(x_ref[...], as_row(n_in_ref[...]))
        pos_col = jnp.transpose(jnp.broadcast_to(pos_row_ref[...].astype(F32), (tokens, tokens)))
        cosine = jnp.zeros((tokens, head_dim), F32)
        sine = jnp.zeros((tokens, head_dim), F32)
        for p in range(cache_len):
            cosine = jnp.where(pos_col == float(p), rope_ref[p:p + 1, :], cosine)
            sine = jnp.where(pos_col == float(p), rope_ref[cache_len + p:cache_len + p + 1, :], sine)

        def rotated(values):
            return values * cosine + pltpu.roll(values, head_dim // 2, 1) * sine

        for head in range(heads):
            pos_s[pl.ds(head, tokens, stride=heads), :] = pos_col
        for load, weights, dest in ((loads[0], wq, q_s), (loads[1], wk, k_s), (loads[2], wv, v_s)):
            load.wait()
            proj = dot_nn(normed, weights[...])
            for head in range(heads):
                values = proj[:, head * head_dim:(head + 1) * head_dim]
                if dest is not v_s:
                    values = rotated(values)
                dest[pl.ds(head, tokens, stride=heads), :] = values.astype(BF16).astype(F32)
            if dest is q_s:
                second_sends()
                for later in loads[3:]:
                    later.start()
        k_new[...] = k_s[...].astype(BF16)
        v_new[...] = v_s[...].astype(BF16)

        for e in range(n_local):
            pltpu.make_async_copy(eg_hbm.at[e], eg.at[e], e_sem.at[0, e]).start()
            pltpu.make_async_copy(eu_hbm.at[e], eu.at[e], e_sem.at[1, e]).start()
            pltpu.make_async_copy(ed_hbm.at[e], ed.at[e], e_sem.at[2, e]).start()

        loads[3].wait()
        loads[4].wait()
        group = 16 // heads
        q_rows, slots = 16, group * cache_len * heads
        shape = (q_rows, slots)
        row, col = lax.broadcasted_iota(jnp.int32, shape, 0), lax.broadcasted_iota(jnp.int32, shape, 1)
        own_rows = jnp.logical_and(row // heads == col // (cache_len * heads), row % heads == col % heads)
        slot = jnp.where(own_rows, col // heads % cache_len, cache_len).astype(F32)

        batch = 8

        def attend(step, carry):
            rows = [pl.ds(pl.multiple_of((step * batch + g) * q_rows, q_rows), q_rows) for g in range(batch)]
            wide_rows = [pl.ds(pl.multiple_of((step * batch + g) * slots, slots), slots) for g in range(batch)]
            query = [q_s[r, :] for r in rows]
            at = [pos_s[r, :] for r in rows]
            scores = [dot_nt(q.astype(BF16), kc[w, :]) * (head_dim ** -0.5) for q, w in zip(query, wide_rows)]
            score_new = [
                jnp.sum(q * k_s[r, :], axis=1, keepdims=True) * (head_dim ** -0.5) for q, r in zip(query, rows)]
            scores = [
                jnp.where(slot < jnp.concatenate([p] * (slots // 128), axis=1), x, -jnp.inf) for x, p in zip(scores, at)]
            top = [jnp.maximum(jnp.max(x, axis=1, keepdims=True), n) for x, n in zip(scores, score_new)]
            weights = [jnp.exp(x - t) for x, t in zip(scores, top)]
            weight_new = [jnp.exp(n - t) for n, t in zip(score_new, top)]
            total = [jnp.sum(w, axis=1, keepdims=True) + n for w, n in zip(weights, weight_new)]
            weights = [(w / t).astype(BF16) for w, t in zip(weights, total)]
            weight_new = [(n / t).astype(BF16).astype(F32) for n, t in zip(weight_new, total)]
            mix = [dot_nn(w, vc[r, :]) for w, r in zip(weights, wide_rows)]
            mix = [m + n * v_s[r, :] for m, n, r in zip(mix, weight_new, rows)]
            for m, r in zip(mix, rows):
                o_s[r, :] = m
            return carry

        n_batches = tokens // group // batch
        lax.fori_loop(0, n_batches // 2, attend, 0)
        for index, onward in ((1, 5), (3, 6)):
            along_y(index)
            along_x(onward)
        lax.fori_loop(n_batches // 2, n_batches, attend, 0)

        mixed = jnp.concatenate(
            [o_s[pl.ds(head, tokens, stride=heads), :] for head in range(heads)], axis=1).astype(BF16)
        loads[5].wait()
        for q in range(n_tp):
            part_q[q] = dot_nn(mixed, wo[:, q * quarter:(q + 1) * quarter]).astype(BF16)
        along_y(2)
        along_y(4)

    pl.run_scoped(
        attention_phase,
        *[pltpu.VMEM((dim, heads * head_dim), BF16)] * 3,
        pltpu.VMEM((heads * head_dim, dim), BF16),
        *[pltpu.VMEM(k_hbm.shape, BF16)] * 2,
        *[pltpu.VMEM((tokens * heads, head_dim), F32)] * 5,
    )

    def attention_sum():
        mine = pl.ds(pl.multiple_of(tp * quarter, quarter), quarter)
        for k in range(1, n_tp):
            arrived(part_in.at[k - 1], a_recv.at[k - 1])
        attn_sum = part_q[tp].astype(F32)
        for k in range(1, n_tp):
            attn_sum = attn_sum + part_in[k - 1].astype(F32)
        h_q[tp] = (x_ref[:, mine].astype(F32) + attn_sum).astype(BF16)
        for k in range(1, n_tp):
            remote(h_q.at[tp], h_q.at[tp], h_send.at[k - 1], h_recv.at[k - 1], tp_peer(k)).start()

    def expert_phase(xs, sort, unsort, z, ys, y_sorted, weight_sorted, place_s, act_s):
        for k in range(1, n_ep):
            source = (ep + n_ep - k) % n_ep
            arrived(all_ids.at[(source % 2) * n_x + source // 2], i_recv.at[k - 1])
        ids = [all_ids[:, k, :] for k in range(2)]
        first = ep * n_local
        lane = lax.broadcasted_iota(jnp.int32, (n_blocks, tokens), 1)
        start = jnp.zeros((n_blocks, tokens), jnp.int32)
        place = jnp.full((n_blocks, tokens), -1, jnp.int32)
        choice = jnp.zeros((n_blocks, tokens), jnp.int32)
        step_expert = jnp.zeros((n_blocks, tokens), jnp.int32)
        step_row = jnp.zeros((n_blocks, tokens), jnp.int32)
        block_row = jnp.zeros((n_blocks, tokens), jnp.int32)
        for e in range(n_local):
            here = [i == first + e for i in ids]
            hit = jnp.where(jnp.logical_or(here[0], here[1]), 1, 0)
            choice = jnp.where(here[1], 1, choice)
            scan = lane_scan(hit)
            totals = jnp.broadcast_to(scan[:, tokens - 1:], scan.shape)
            above = row_scan(totals)
            count = jnp.broadcast_to(above[n_blocks - 1:, :], scan.shape)
            place = jnp.where(hit == 1, start + above - totals + scan - 1, place)
            step_row = jnp.where(lane == e, start, step_row)
            step_expert = jnp.where(lane == e, e, step_expert)
            spill = jnp.logical_and(lane == n_local, count > ROWS)
            step_row = jnp.where(spill, start + ROWS, step_row)
            step_expert = jnp.where(spill, e, step_expert)
            later = start + (count + ALIGN - 1) // ALIGN * ALIGN
            into = lane * ALIGN - start
            inside = jnp.logical_and(into >= 0, lane * ALIGN < later)
            block_row = jnp.where(
                inside, jnp.where(into < ROWS, e * ROWS + into, n_local * ROWS + into - ROWS), block_row)
            start = later
        step_row = jnp.minimum(step_row, n_sorted)
        block_row = jnp.minimum(block_row, n_steps * ROWS - ALIGN)
        table_row = lax.broadcasted_iota(jnp.int32, (n_blocks, tokens), 0)
        sched_v[...] = jnp.where(
            table_row == 0, step_expert, jnp.where(table_row == 1, step_row // ALIGN, block_row // ALIGN))
        to_scalar = pltpu.make_async_copy(sched_v, sched, w_sem.at[8])
        to_scalar.start()

        place_s[...] = place
        row_id = lax.broadcasted_iota(jnp.int32, (n_sorted, tokens), 0)
        groups = (
            ((core, chip), (other, chip)), ((core, left), (core, right)), ((other, left), (other, right)),
            ((core, far), (other, far)))
        for n, pair in enumerate(groups):
            for m, (c, spot) in enumerate(pair):
                match = row_id == place_s[pl.ds(c * n_x + spot, 1), :]
                first_col = (2 * n + m) * tokens
                sort[:, first_col:first_col + tokens] = jnp.where(match, 1.0, 0.0).astype(BF16)

        def sort_weights():
            for k in range(1, n_ep):
                source = (ep + n_ep - k) % n_ep
                arrived(meta.at[(source % 2) * n_x + source // 2], m_recv.at[k - 1])
            weight = jnp.where(choice == 1, meta[:, 1, :], meta[:, 0, :])
            weight_rows = jnp.zeros((n_sorted, tokens), F32)
            for j in range(n_blocks):
                weight_rows = weight_rows + jnp.where(row_id == place[j:j + 1, :], weight[j:j + 1, :], 0.0)
            weight_sorted[0:n_sorted, :] = jnp.broadcast_to(
                jnp.sum(weight_rows, axis=1, keepdims=True), (n_sorted, 128))
            weight_sorted[n_sorted:, :] = jnp.zeros((ROWS, 128), F32)

        xs[n_sorted:, :] = jnp.zeros((ROWS, dim), BF16)
        def add_rows(n):
            def one(i, carry):
                cols = pl.ds(pl.multiple_of(i * 256, 256), 256)
                rows = jnp.concatenate([rows_all[c, spot, :, cols] for c, spot in groups[n]], axis=0)
                total = dot_nn(sort[:, 2 * n * tokens:(2 * n + 2) * tokens], rows)
                if n > 0:
                    total = total + xs[0:n_sorted, cols].astype(F32)
                xs[0:n_sorted, cols] = total.astype(BF16)
                return carry

            lax.fori_loop(0, dim // 256, one, 0, unroll=2)

        arrived(rows_all.at[other, chip], ag_recv.at[0])
        add_rows(0)
        along_y(5)
        along_y(6)
        for index in (1, 3, 2, 4):
            across(index)
        add_rows(1)
        for index in (5, 6):
            across(index)
        for k in range(1, n_tp):
            remote(part_q.at[(tp + k) % n_tp], part_in.at[k - 1], a_send.at[k - 1], a_recv.at[k - 1], tp_peer(k)).start()
        place_cols = jnp.transpose(place.astype(F32))
        column_id = lax.broadcasted_iota(jnp.int32, (tokens, n_sorted), 1).astype(F32)
        for j in range(n_blocks):
            unsort[j * tokens:(j + 1) * tokens, :] = jnp.where(
                column_id == place_cols[:, j:j + 1], 1.0, 0.0).astype(BF16)
        sort_weights()
        for index in (1, 3, 2, 4):
            arrived_across(index)
        add_rows(2)
        for index in (5, 6):
            arrived_across(index)
        add_rows(3)
        for index in messages:
            sent(rows_all.at[core, chip, low, side], ag_send.at[index])
            sent(rows_all.at[core, chip, low, side], y_send.at[index - 1])
            sent(rows_all.at[core, chip, low], ag_send.at[index + 6])
        sent(rows_all.at[core, chip], ag_send.at[0])
        for k in range(1, n_ep):
            sent(meta.at[core * n_x + chip], m_send.at[k - 1])
            sent(all_ids.at[core * n_x + chip], i_send.at[k - 1])
        to_scalar.wait()
        for e in range(n_local):
            pltpu.make_async_copy(eg_hbm.at[e], eg.at[e], e_sem.at[0, e]).wait()
            pltpu.make_async_copy(eu_hbm.at[e], eu.at[e], e_sem.at[1, e]).wait()

        def gate_up(step, carry):
            e = sched[0, step]
            rows = xs[pl.ds(sched[1, step] * ALIGN, ROWS), :]
            act = jax.nn.silu(dot_nt(eg[e], rows)) * dot_nt(eu[e], rows)
            z[step] = jnp.transpose(act).astype(BF16)
            return carry

        lax.fori_loop(0, n_steps, gate_up, 0, unroll=3)

        for p in range(dense_parts):
            pltpu.make_async_copy(wg_hbm.at[p], eg.at[p], w_sem.at[p]).start()
            pltpu.make_async_copy(wu_hbm.at[p], eu.at[p], w_sem.at[2 + p]).start()
            pltpu.make_async_copy(wd_hbm.at[p], eg.at[dense_parts + p], w_sem.at[4 + p]).start()
        for e in range(n_local):
            pltpu.make_async_copy(ed_hbm.at[e], ed.at[e], e_sem.at[2, e]).wait()

        def results(i):
            cols = columns(i)

            def down(step, carry):
                e = sched[0, step]
                scale = weight_sorted[pl.ds(sched[1, step] * ALIGN, ROWS), :]
                prod = dot_nn(z[step], ed[e, :, cols])
                scaled = [prod[:, b * 128:(b + 1) * 128] * scale for b in range(quarter // 128)]
                ys[pl.ds(pl.multiple_of(step * ROWS, ROWS), ROWS), :] = jnp.concatenate(scaled, axis=1).astype(BF16)
                return carry

            lax.fori_loop(0, n_steps, down, 0, unroll=3)

            def regroup(b, carry):
                y_sorted[pl.ds(pl.multiple_of(b * ALIGN, ALIGN), ALIGN), :] = ys[pl.ds(sched[2, b] * ALIGN, ALIGN), :]
                return carry

            lax.fori_loop(0, n_sorted // ALIGN, regroup, 0, unroll=8)

        def to_tokens(i):
            cols = columns(i)
            for c in range(2):
                back = dot_nn(unsort[c * n_x * tokens:(c + 1) * n_x * tokens, :], y_sorted[...])
                rows_all[c, :, :, cols] = back.astype(BF16).reshape(n_x, tokens, quarter)
            remote(rows_all.at[other, :, :, cols], d_in.at[i], d_send.at[i], d_recv.at[i], partner).start()

        attention_sum()
        results(0)
        to_tokens(0)
        results(1)
        pair_sum(0)
        pair_sum_rest(0)
        to_tokens(1)
        results(2)
        pair_sum(1)
        pair_sum_rest(1)
        to_tokens(2)
        ring_sum(0)
        results(3)
        pair_sum(2)
        pair_sum_rest(2)
        to_tokens(3)
        ring_sum(1)
        pair_sum(3)
        ring_sum(2)
        dense_gate_up(act_s)
        pair_sum_rest(3)
        dense_down(act_s)
        ring_sum(3)
        finish(0)
        finish(1)
        finish(2)
        finish(3)

    def columns(i):
        return pl.ds(pl.multiple_of(((tp + 1 + i) % n_tp) * quarter, quarter), quarter)

    def pair_sum(i):
        cols = columns(i)
        arrived(d_in.at[i], d_recv.at[i])
        for spot in range(n_x):
            rows_all[core, spot, :, cols] = (
                rows_all[core, spot, :, cols].astype(F32) + d_in[i, spot].astype(F32)).astype(BF16)
        remote(rows_all.at[core, far, low, cols], r1_in.at[i, 0], r1_send.at[i, 0], r1_recv.at[i, 0], on_ring(right)).start()
        remote(rows_all.at[core, far, high, cols], r1_in.at[i, 1], r1_send.at[i, 1], r1_recv.at[i, 1], on_ring(left)).start()

    def pair_sum_rest(i):
        cols = columns(i)
        remote(rows_all.at[core, right, high, cols], r2_in.at[i, 0, high], r2_send.at[i, 0], r2_recv.at[i, 0], on_ring(right)).start()
        remote(rows_all.at[core, left, low, cols], r2_in.at[i, 1, low], r2_send.at[i, 1], r2_recv.at[i, 1], on_ring(left)).start()

    def ring_sum(i):
        cols = columns(i)
        arrived(r1_in.at[i, 0], r1_recv.at[i, 0])
        rows_all[core, right, low, cols] = (
            rows_all[core, right, low, cols].astype(F32) + r1_in[i, 0].astype(F32)).astype(BF16)
        remote(rows_all.at[core, right, low, cols], r2_in.at[i, 0, low], r2_send.at[i, 2], r2_recv.at[i, 2], on_ring(right)).start()
        arrived(r1_in.at[i, 1], r1_recv.at[i, 1])
        rows_all[core, left, high, cols] = (
            rows_all[core, left, high, cols].astype(F32) + r1_in[i, 1].astype(F32)).astype(BF16)
        remote(rows_all.at[core, left, high, cols], r2_in.at[i, 1, high], r2_send.at[i, 3], r2_recv.at[i, 3], on_ring(left)).start()

    def dense_gate_up(act_s):
        for k in range(1, n_tp):
            source = (tp + n_tp - k) % n_tp
            arrived(h_q.at[source], h_recv.at[k - 1])
        hidden_mid = jnp.concatenate([h_q[q] for q in range(n_tp)], axis=1)
        c_buf[...] = rms_norm(hidden_mid, as_row(n_res_ref[...]))
        for p in range(dense_parts):
            pltpu.make_async_copy(wg_hbm.at[p], eg.at[p], w_sem.at[p]).wait()
            pltpu.make_async_copy(wu_hbm.at[p], eu.at[p], w_sem.at[2 + p]).wait()
            act = jax.nn.silu(dot_nt(eg[p], c_buf[...])) * dot_nt(eu[p], c_buf[...])
            act_s[p] = jnp.transpose(act).astype(BF16)

    def dense_down(act_s):
        for p in range(dense_parts):
            pltpu.make_async_copy(wd_hbm.at[p], eg.at[dense_parts + p], w_sem.at[4 + p]).wait()
        for q in range(n_tp):
            cols = slice(q * quarter, (q + 1) * quarter)
            dense = dot_nn(act_s[0], eg[dense_parts, :, cols])
            for p in range(1, dense_parts):
                dense = dense + dot_nn(act_s[p], eg[dense_parts + p, :, cols])
            dense_q[q] = dense

    def finish(i):
        q = (tp + 1 + i) % n_tp
        cols = columns(i)
        arrived(r2_in.at[i, 0, high], r2_recv.at[i, 0])
        arrived(r2_in.at[i, 1, low], r2_recv.at[i, 1])
        arrived(r2_in.at[i, 0, low], r2_recv.at[i, 2])
        arrived(r2_in.at[i, 1, high], r2_recv.at[i, 3])
        part = rows_all[core, chip, :, cols].astype(F32) + r2_in[i, 0].astype(F32) + r2_in[i, 1].astype(F32) + dense_q[q]
        if i < n_tp - 1:
            fin_q[i] = part.astype(BF16)
            remote(fin_q.at[i], fin_in.at[i], f_send.at[i], f_recv.at[i], tp_peer(i + 1)).start()
        else:
            for k in range(1, n_tp):
                arrived(fin_in.at[k - 1], f_recv.at[k - 1])
                part = part + fin_in[k - 1].astype(F32)
            out_q[tp] = (h_q[tp].astype(F32) + part).astype(BF16)

    pl.run_scoped(
        expert_phase,
        pltpu.VMEM((n_sorted + ROWS, dim), BF16),
        pltpu.VMEM((n_sorted, all_rows), BF16),
        pltpu.VMEM((all_rows, n_sorted), BF16),
        pltpu.VMEM((n_steps, ROWS, width), BF16),
        pltpu.VMEM((n_steps * ROWS, quarter), BF16),
        pltpu.VMEM((n_sorted, quarter), BF16),
        pltpu.VMEM((n_sorted + ROWS, 128), F32),
        pltpu.VMEM((n_blocks, tokens), jnp.int32),
        pltpu.VMEM((dense_parts, tokens, width), BF16),
    )
    before, after, opposite = (tp + n_tp - 1) % n_tp, (tp + 1) % n_tp, (tp + 2) % n_tp
    up, down = tp_peer(1), tp_peer(n_tp - 1)

    def pass_on(index, place, rows, device):
        block = out_q.at[place, rows]
        remote(block, block, o_send.at[index], o_recv.at[index], device).start()

    pass_on(0, tp, low, up)
    pass_on(1, tp, high, down)
    out_ref[:, pl.ds(pl.multiple_of(tp * quarter, quarter), quarter)] = out_q[tp]
    for index in range(2):
        sent(out_q.at[tp, low], o_send.at[index])
    pass_on(2, tp, high, up)
    pass_on(3, tp, low, down)
    arrived(out_q.at[before, low], o_recv.at[0])
    pass_on(4, before, low, up)
    arrived(out_q.at[after, high], o_recv.at[1])
    pass_on(5, after, high, down)

    for i in range(n_tp):
        cols = columns(i)
        sent(d_in.at[i], d_send.at[i])
        for side in range(2):
            sent(r1_in.at[i, side], r1_send.at[i, side])
        for message in range(4):
            sent(r1_in.at[i, 0], r2_send.at[i, message])
    for k in range(1, n_tp):
        sent(part_in.at[k - 1], a_send.at[k - 1])
        sent(part_in.at[k - 1], h_send.at[k - 1])
        sent(part_in.at[k - 1], f_send.at[k - 1])
    arrived(out_q.at[before, high], o_recv.at[2])
    arrived(out_q.at[after, low], o_recv.at[3])
    for place in (before, after):
        out_ref[:, pl.ds(pl.multiple_of(place * quarter, quarter), quarter)] = out_q[place]
    arrived(out_q.at[opposite, low], o_recv.at[4])
    arrived(out_q.at[opposite, high], o_recv.at[5])
    out_ref[:, pl.ds(pl.multiple_of(opposite * quarter, quarter), quarter)] = out_q[opposite]
    for index in range(2, 6):
        sent(out_q.at[tp, low], o_send.at[index])


def cache_kernel(pieces, pos, hidden, k_new_hbm, v_new_hbm, k_hbm, v_hbm, out, k_out, v_out, hidden_buf, k_new, v_new, k_buf, v_buf, in_sem, out_sem, sem):
    size = k_buf.shape[0] // pieces
    both = ((k_hbm, k_buf, k_out, k_new), (v_hbm, v_buf, v_out, v_new))
    first = [
        pltpu.make_async_copy(k_new_hbm, k_new, sem.at[0]),
        pltpu.make_async_copy(v_new_hbm, v_new, sem.at[1]),
    ]
    hidden_in, hidden_out = (
        pltpu.make_async_copy(hidden, hidden_buf, sem.at[2]), pltpu.make_async_copy(hidden_buf, out, sem.at[3]))
    loads = [
        [pltpu.make_async_copy(src.at[pl.ds(i * size, size)], buf.at[pl.ds(i * size, size)], in_sem.at[n, i])
         for n, (src, buf, _, _) in enumerate(both)] for i in range(pieces)]
    stores = [
        [pltpu.make_async_copy(buf.at[pl.ds(i * size, size)], dst.at[pl.ds(i * size, size)], out_sem.at[n, i])
         for n, (_, buf, dst, _) in enumerate(both)] for i in range(pieces)]
    for load in first:
        load.start()
    for pair in loads:
        for load in pair:
            load.start()
    hidden_in.start()
    for load in first:
        load.wait()
    for i in range(pieces):
        for n, (_, buf, _, new) in enumerate(both):
            loads[i][n].wait()
            for t in range(i * size, (i + 1) * size):
                buf[t, pos[t]] = new[t]
            stores[i][n].start()
    hidden_in.wait()
    hidden_out.start()
    for pair in stores:
        for store in pair:
            store.wait()
    hidden_out.wait()


def rope_table(cache_len, head_dim):
    freq = 1.0 / (ROPE_BASE ** (np.arange(0, head_dim, 2, dtype=np.float32) / np.float32(head_dim)))
    angle = np.arange(cache_len, dtype=np.float32)[:, None] * freq.astype(np.float32)[None, :]
    cosine, sine = np.cos(angle), np.sin(angle)
    return np.concatenate(
        [np.concatenate([cosine, cosine], 1), np.concatenate([-sine, sine], 1)], 0).astype(np.float32)


def solution(mesh):
    n_tp, n_ep = mesh.shape['tp'], mesh.shape['ep']
    row_spec = P(('dp', 'ep'), None)
    cache_spec = P(('dp', 'ep'), None, 'tp', None)
    col_split = P(None, 'tp')
    row_split = P('tp', None)
    in_specs = (row_spec, P(('dp', 'ep')), row_spec, cache_spec, cache_spec, P(None), P(None), P(None), col_split, col_split, col_split, row_split, col_split, col_split, row_split, P(None, None), P('ep', None, 'tp'), P('ep', None, 'tp'), P('ep', 'tp', None))
    out_specs = (row_spec, cache_spec, cache_spec)

    def local_layer(hidden_in, positions, expert_ids, k_cache, v_cache, norm_in, norm_res, norm_post, w_q, w_k, w_v, w_o, w_gate, w_up, w_down, w_router, e_gate, e_up, e_down):
        tokens, dim = hidden_in.shape
        n_local, width = e_gate.shape[0], e_gate.shape[2]
        cache_len, heads, head_dim = k_cache.shape[1:]
        dense_parts = w_down.shape[0] // width
        quarter = dim // n_tp
        n_x = n_ep // 2
        half = tokens // 2
        vmem = pl.BlockSpec(memory_space=pltpu.VMEM)
        hbm = pl.BlockSpec(memory_space=pl.ANY)
        dma = pltpu.SemaphoreType.DMA
        hidden, k_new, v_new = pl.pallas_call(
            functools.partial(layer_kernel, n_tp, n_ep, 'ep', 'tp'),
            out_shape=(
                jax.ShapeDtypeStruct(hidden_in.shape, BF16),
                jax.ShapeDtypeStruct((tokens * heads, head_dim), BF16),
                jax.ShapeDtypeStruct((tokens * heads, head_dim), BF16),
            ),
            in_specs=[vmem] * 8 + [hbm] * 12,
            out_specs=(vmem, vmem, vmem),
            scratch_shapes=[
                pltpu.VMEM((n_local, width, dim), BF16),
                pltpu.VMEM((n_local, width, dim), BF16),
                pltpu.VMEM((n_local, width, dim), BF16),
                pltpu.VMEM((2, n_x, tokens, dim), BF16),
                pltpu.VMEM((n_ep, 8, tokens), F32),
                pltpu.VMEM((n_ep, 8, tokens), jnp.int32),
                pltpu.VMEM((n_tp, tokens, quarter), BF16),
                pltpu.VMEM((n_tp - 1, tokens, quarter), BF16),
                pltpu.VMEM((n_tp, tokens, quarter), BF16),
                pltpu.VMEM((tokens, dim), BF16),
                pltpu.VMEM((n_tp, n_x, tokens, quarter), BF16),
                pltpu.VMEM((n_tp, 2, half, quarter), BF16),
                pltpu.VMEM((n_tp, 2, tokens, quarter), BF16),
                pltpu.VMEM((n_tp, tokens, quarter), F32),
                pltpu.VMEM((n_tp - 1, tokens, quarter), BF16),
                pltpu.VMEM((n_tp - 1, tokens, quarter), BF16),
                pltpu.VMEM((n_tp, tokens, quarter), BF16),
                pltpu.VMEM((n_ep, tokens), jnp.int32),
                pltpu.SMEM((n_ep, tokens), jnp.int32),
                dma((9,)), dma((3, n_local)), dma((13,)), dma((13,)), *[dma((n_ep - 1,))] * 4, dma((6,)), dma((6,)),
                *[dma((n_tp - 1,))] * 4,
                dma((n_tp,)), dma((n_tp,)),
                dma((n_tp, 2)), dma((n_tp, 2)), dma((n_tp, 4)), dma((n_tp, 4)),
                *[dma((n_tp - 1,))] * 2, dma((6,)), dma((6,)),
            ],
            compiler_params=pltpu.CompilerParams(
                collective_id=0, has_side_effects=True, vmem_limit_bytes=67043328),
        )(
            hidden_in, positions.reshape(1, tokens), expert_ids.T,
            norm_in.reshape(-1, 128), norm_res.reshape(-1, 128), norm_post.reshape(-1, 128), w_router.T,
            jnp.asarray(rope_table(cache_len, head_dim)),
            k_cache.reshape(-1, head_dim), v_cache.reshape(-1, head_dim), w_q, w_k, w_v, w_o,
            w_gate.T.reshape(dense_parts, width, dim), w_up.T.reshape(dense_parts, width, dim),
            w_down.reshape(dense_parts, width, dim),
            jnp.swapaxes(e_gate, 1, 2), jnp.swapaxes(e_up, 1, 2), e_down,
        )
        return pl.pallas_call(
            functools.partial(cache_kernel, 8),
            out_shape=(
                jax.ShapeDtypeStruct(hidden_in.shape, BF16),
                jax.ShapeDtypeStruct(k_cache.shape, BF16),
                jax.ShapeDtypeStruct(v_cache.shape, BF16),
            ),
            in_specs=[pl.BlockSpec(memory_space=pltpu.SMEM)] + [hbm] * 5,
            out_specs=(hbm, hbm, hbm),
            scratch_shapes=[
                pltpu.VMEM(hidden_in.shape, BF16),
                pltpu.VMEM((tokens, heads, head_dim), BF16), pltpu.VMEM((tokens, heads, head_dim), BF16),
                pltpu.VMEM(k_cache.shape, BF16), pltpu.VMEM(v_cache.shape, BF16),
                dma((2, 8)), dma((2, 8)), dma((4,)),
            ],
        )(positions, hidden, k_new.reshape(tokens, heads, head_dim), v_new.reshape(tokens, heads, head_dim), k_cache, v_cache)

    return jax.shard_map(local_layer, mesh=mesh, in_specs=in_specs, out_specs=out_specs, check_vma=False)
```

```python
import functools

import jax
import jax.numpy as jnp
import numpy as np
from jax import lax
from jax.experimental import pallas as pl
from jax.experimental.pallas import tpu as pltpu
from jax.sharding import PartitionSpec as P

NORM_EPS = 1e-5
ROPE_BASE = 10000.0
F32 = jnp.float32
BF16 = jnp.bfloat16
MESH = pl.DeviceIdType.MESH
ROWS = 256
ALIGN = 16


def as_row(gains):
    wide = gains.astype(F32)
    return jnp.concatenate([wide[i:i + 1, :] for i in range(wide.shape[0])], axis=1)


def rms_norm(values, gain_row):
    wide_vals = values.astype(F32)
    inv_rms = lax.rsqrt(jnp.mean(wide_vals * wide_vals, axis=-1, keepdims=True) + NORM_EPS)
    return (wide_vals * inv_rms * gain_row.astype(F32)).astype(BF16)


def dot_nn(a, b):
    return lax.dot_general(a, b, (((1,), (0,)), ((), ())), preferred_element_type=F32)


def dot_nt(a, b):
    return lax.dot_general(a, b, (((1,), (1,)), ((), ())), preferred_element_type=F32)


def lane_scan(values):
    lane = lax.broadcasted_iota(jnp.int32, values.shape, 1)
    step = 1
    while step < values.shape[1]:
        values = values + jnp.where(lane >= step, pltpu.roll(values, step, 1), 0)
        step *= 2
    return values


def row_scan(values):
    row = lax.broadcasted_iota(jnp.int32, values.shape, 0)
    step = 1
    while step < values.shape[0]:
        values = values + jnp.where(row >= step, pltpu.roll(values, step, 0), 0)
        step *= 2
    return values


def layer_kernel(
    n_tp, n_ep, ep_axis, tp_axis,
    x_ref, pos_row_ref, ids_ref, n_in_ref, n_res_ref, n_post_ref, w_router_ref, rope_ref,
    k_hbm, v_hbm, wq_hbm, wk_hbm, wv_hbm, wo_hbm, wg_hbm, wu_hbm, wd_hbm, eg_hbm, eu_hbm, ed_hbm,
    out_ref, k_new, v_new,
    eg, eu, ed, rows_all, meta, all_ids, part_q, part_in, h_q, c_buf, d_in, r1_in, r2_in, dense_q, fin_q, fin_in, out_q,
    sched_v, sched,
    w_sem, e_sem, ag_send, ag_recv, m_send, m_recv, i_send, i_recv, y_send, y_recv, a_send, a_recv, h_send, h_recv, d_send, d_recv,
    r1_send, r1_recv, r2_send, r2_recv, f_send, f_recv, o_send, o_recv,
):
    tokens, dim = x_ref.shape
    quarter = dim // n_tp
    n_x = n_ep // 2
    half = tokens // 2
    n_local, width = eg.shape[0], eg.shape[1]
    head_dim = k_hbm.shape[1]
    heads = wq_hbm.shape[1] // head_dim
    cache_len = k_hbm.shape[0] // (tokens * heads)
    n_blocks = n_ep
    all_rows = n_blocks * tokens
    n_sorted = -(-(4 * tokens + n_local * (ALIGN - 1)) // 128) * 128
    n_steps = n_local + 1
    dense_parts = wd_hbm.shape[0]

    ep = lax.axis_index(ep_axis)
    tp = lax.axis_index(tp_axis)
    chip = ep // 2
    core = ep % 2
    other = 1 - core
    right = (chip + 1) % n_x
    left = (chip + n_x - 1) % n_x
    far = (chip + 2) % n_x

    def on_ring(place):
        return {ep_axis: place * 2 + core}

    partner = {ep_axis: chip * 2 + other}

    def ep_peer(k):
        return {ep_axis: (ep + k) % n_ep}

    def tp_peer(k):
        return {tp_axis: (tp + k) % n_tp}

    def remote(src, dst, send_sem, recv_sem, device):
        return pltpu.make_async_remote_copy(
            src_ref=src, dst_ref=dst, send_sem=send_sem, recv_sem=recv_sem, device_id=device, device_id_type=MESH)

    def arrived(dst, recv_sem):
        remote(dst, dst, recv_sem, recv_sem, partner).wait_recv()

    def sent(src, send_sem):
        remote(src, src, send_sem, send_sem, partner).wait_send()

    low, high = pl.ds(0, half), pl.ds(half, half)

    messages = {1: (left, low), 2: (left, high), 3: (right, high), 4: (right, low), 5: (far, low), 6: (far, high)}
    side = pl.ds(pl.multiple_of((tp % 2) * (dim // 2), dim // 2), dim // 2)
    side_in = pl.ds(pl.multiple_of((1 - tp % 2) * (dim // 2), dim // 2), dim // 2)

    def along_x(index):
        place = {5: left, 6: right}.get(index, chip)
        rows = messages[index][1]
        block = rows_all.at[core, place, rows, side]
        device = on_ring(right if index in (1, 2, 5) else left)
        remote(block, block, ag_send.at[index], ag_recv.at[index], device).start()

    def along_y(index):
        place, rows = messages[index]
        block = rows_all.at[core, place, rows, side]
        arrived(block, ag_recv.at[index])
        device = tp_peer(1) if rows is low else tp_peer(n_tp - 1)
        remote(block, block, y_send.at[index - 1], y_recv.at[index - 1], device).start()

    def across(index):
        place, rows = messages[index]
        arrived(rows_all.at[core, place, rows, side_in], y_recv.at[index - 1])
        block = rows_all.at[core, place, rows]
        remote(block, block, ag_send.at[index + 6], ag_recv.at[index + 6], partner).start()

    def arrived_across(index):
        place, rows = messages[index]
        arrived(rows_all.at[other, place, rows], ag_recv.at[index + 6])

    barrier = pltpu.get_barrier_semaphore()
    for k in range(1, n_ep):
        pl.semaphore_signal(barrier, inc=1, device_id=ep_peer(k), device_id_type=MESH)
    for k in range(1, n_tp):
        pl.semaphore_signal(barrier, inc=1, device_id=tp_peer(k), device_id_type=MESH)

    def attention_phase(wq, wk, wv, wo, kc, vc, q_s, k_s, v_s, o_s, pos_s):
        loads = [
            pltpu.make_async_copy(src, dst, w_sem.at[i])
            for i, (src, dst) in enumerate(
                ((wq_hbm, wq), (wk_hbm, wk), (wv_hbm, wv), (k_hbm, kc), (v_hbm, vc), (wo_hbm, wo)))
        ]
        loads[0].start()

        for later in loads[1:]:
            later.start()

        moe_in = rms_norm(x_ref[...], as_row(n_post_ref[...]))
        rows_all[core, chip] = moe_in
        ids = ids_ref[...]
        all_ids[core * n_x + chip] = jnp.concatenate([ids, jnp.zeros((6, tokens), jnp.int32)], axis=0)
        pl.semaphore_wait(barrier, n_ep - 1 + n_tp - 1)
        for k in range(1, n_ep):
            block = all_ids.at[core * n_x + chip]
            remote(block, block, i_send.at[k - 1], i_recv.at[k - 1], ep_peer(k)).start()
        along_x(1)
        along_x(3)
        own = rows_all.at[core, chip]
        remote(own, own, ag_send.at[0], ag_recv.at[0], partner).start()
        logits = dot_nt(w_router_ref[...], moe_in)
        shifted = jnp.exp(logits - jnp.max(logits, axis=0, keepdims=True))
        probs = shifted / jnp.sum(shifted, axis=0, keepdims=True)
        expert_row = lax.broadcasted_iota(jnp.int32, probs.shape, 0)
        picked = [
            jnp.sum(jnp.where(expert_row == ids[k:k + 1, :], probs, 0.0), axis=0, keepdims=True) for k in range(2)
        ]
        total = picked[0] + picked[1]
        meta[core * n_x + chip] = jnp.concatenate(
            [picked[0] / total, picked[1] / total, jnp.zeros((6, tokens), F32)], axis=0)

        def second_sends():
            along_x(2)
            along_x(4)
            for k in range(1, n_ep):
                block = meta.at[core * n_x + chip]
                remote(block, block, m_send.at[k - 1], m_recv.at[k - 1], ep_peer(k)).start()

        normed = rms_norm(x_ref[...], as_row(n_in_ref[...]))
        pos_col = jnp.transpose(jnp.broadcast_to(pos_row_ref[...].astype(F32), (tokens, tokens)))
        cosine = jnp.zeros((tokens, head_dim), F32)
        sine = jnp.zeros((tokens, head_dim), F32)
        for p in range(cache_len):
            cosine = jnp.where(pos_col == float(p), rope_ref[p:p + 1, :], cosine)
            sine = jnp.where(pos_col == float(p), rope_ref[cache_len + p:cache_len + p + 1, :], sine)

        def rotated(values):
            return values * cosine + pltpu.roll(values, head_dim // 2, 1) * sine

        for head in range(heads):
            pos_s[pl.ds(head, tokens, stride=heads), :] = pos_col
        for load, weights, dest in ((loads[0], wq, q_s), (loads[1], wk, k_s), (loads[2], wv, v_s)):
            load.wait()
            proj = dot_nn(normed, weights[...])
            for head in range(heads):
                values = proj[:, head * head_dim:(head + 1) * head_dim]
                if dest is not v_s:
                    values = rotated(values)
                dest[pl.ds(head, tokens, stride=heads), :] = values.astype(BF16).astype(F32)
            if dest is q_s:
                second_sends()
        k_new[...] = k_s[...].astype(BF16)
        v_new[...] = v_s[...].astype(BF16)

        for e in range(n_local):
            pltpu.make_async_copy(eg_hbm.at[e], eg.at[e], e_sem.at[0, e]).start()
            pltpu.make_async_copy(eu_hbm.at[e], eu.at[e], e_sem.at[1, e]).start()
            pltpu.make_async_copy(ed_hbm.at[e], ed.at[e], e_sem.at[2, e]).start()

        loads[3].wait()
        loads[4].wait()
        group = 16 // heads
        q_rows, slots = 16, group * cache_len * heads
        shape = (q_rows, slots)
        row, col = lax.broadcasted_iota(jnp.int32, shape, 0), lax.broadcasted_iota(jnp.int32, shape, 1)
        own_rows = jnp.logical_and(row // heads == col // (cache_len * heads), row % heads == col % heads)
        slot = jnp.where(own_rows, col // heads % cache_len, cache_len).astype(F32)

        batch = 8

        def attend(step, carry):
            rows = [pl.ds(pl.multiple_of((step * batch + g) * q_rows, q_rows), q_rows) for g in range(batch)]
            wide_rows = [pl.ds(pl.multiple_of((step * batch + g) * slots, slots), slots) for g in range(batch)]
            query = [q_s[r, :] for r in rows]
            at = [pos_s[r, :] for r in rows]
            scores = [dot_nt(q.astype(BF16), kc[w, :]) * (head_dim ** -0.5) for q, w in zip(query, wide_rows)]
            score_new = [
                jnp.sum(q * k_s[r, :], axis=1, keepdims=True) * (head_dim ** -0.5) for q, r in zip(query, rows)]
            scores = [
                jnp.where(slot < jnp.concatenate([p] * (slots // 128), axis=1), x, -jnp.inf) for x, p in zip(scores, at)]
            top = [jnp.maximum(jnp.max(x, axis=1, keepdims=True), n) for x, n in zip(scores, score_new)]
            weights = [jnp.exp(x - t) for x, t in zip(scores, top)]
            weight_new = [jnp.exp(n - t) for n, t in zip(score_new, top)]
            total = [jnp.sum(w, axis=1, keepdims=True) + n for w, n in zip(weights, weight_new)]
            weights = [(w / t).astype(BF16) for w, t in zip(weights, total)]
            weight_new = [(n / t).astype(BF16).astype(F32) for n, t in zip(weight_new, total)]
            mix = [dot_nn(w, vc[r, :]) for w, r in zip(weights, wide_rows)]
            mix = [m + n * v_s[r, :] for m, n, r in zip(mix, weight_new, rows)]
            for m, r in zip(mix, rows):
                o_s[r, :] = m
            return carry

        lax.fori_loop(0, tokens // group // batch, attend, 0)
        for index, onward in ((1, 5), (3, 6)):
            along_y(index)
            along_x(onward)

        mixed = jnp.concatenate(
            [o_s[pl.ds(head, tokens, stride=heads), :] for head in range(heads)], axis=1).astype(BF16)
        loads[5].wait()
        for q in range(n_tp):
            part_q[q] = dot_nn(mixed, wo[:, q * quarter:(q + 1) * quarter]).astype(BF16)
        along_y(2)
        along_y(4)

    pl.run_scoped(
        attention_phase,
        *[pltpu.VMEM((dim, heads * head_dim), BF16)] * 3,
        pltpu.VMEM((heads * head_dim, dim), BF16),
        *[pltpu.VMEM(k_hbm.shape, BF16)] * 2,
        *[pltpu.VMEM((tokens * heads, head_dim), F32)] * 5,
    )

    def attention_sum():
        mine = pl.ds(pl.multiple_of(tp * quarter, quarter), quarter)
        for k in range(1, n_tp):
            arrived(part_in.at[k - 1], a_recv.at[k - 1])
        attn_sum = part_q[tp].astype(F32)
        for k in range(1, n_tp):
            attn_sum = attn_sum + part_in[k - 1].astype(F32)
        h_q[tp] = (x_ref[:, mine].astype(F32) + attn_sum).astype(BF16)
        for k in range(1, n_tp):
            remote(h_q.at[tp], h_q.at[tp], h_send.at[k - 1], h_recv.at[k - 1], tp_peer(k)).start()

    def expert_phase(xs, sort, unsort, z, ys, y_sorted, weight_sorted, place_s, act_s):
        for k in range(1, n_ep):
            source = (ep + n_ep - k) % n_ep
            arrived(all_ids.at[(source % 2) * n_x + source // 2], i_recv.at[k - 1])
        ids = [all_ids[:, k, :] for k in range(2)]
        first = ep * n_local
        lane = lax.broadcasted_iota(jnp.int32, (n_blocks, tokens), 1)
        start = jnp.zeros((n_blocks, tokens), jnp.int32)
        place = jnp.full((n_blocks, tokens), -1, jnp.int32)
        choice = jnp.zeros((n_blocks, tokens), jnp.int32)
        step_expert = jnp.zeros((n_blocks, tokens), jnp.int32)
        step_row = jnp.zeros((n_blocks, tokens), jnp.int32)
        block_row = jnp.zeros((n_blocks, tokens), jnp.int32)
        for e in range(n_local):
            here = [i == first + e for i in ids]
            hit = jnp.where(jnp.logical_or(here[0], here[1]), 1, 0)
            choice = jnp.where(here[1], 1, choice)
            scan = lane_scan(hit)
            totals = jnp.broadcast_to(scan[:, tokens - 1:], scan.shape)
            above = row_scan(totals)
            count = jnp.broadcast_to(above[n_blocks - 1:, :], scan.shape)
            place = jnp.where(hit == 1, start + above - totals + scan - 1, place)
            step_row = jnp.where(lane == e, start, step_row)
            step_expert = jnp.where(lane == e, e, step_expert)
            spill = jnp.logical_and(lane == n_local, count > ROWS)
            step_row = jnp.where(spill, start + ROWS, step_row)
            step_expert = jnp.where(spill, e, step_expert)
            later = start + (count + ALIGN - 1) // ALIGN * ALIGN
            into = lane * ALIGN - start
            inside = jnp.logical_and(into >= 0, lane * ALIGN < later)
            block_row = jnp.where(
                inside, jnp.where(into < ROWS, e * ROWS + into, n_local * ROWS + into - ROWS), block_row)
            start = later
        step_row = jnp.minimum(step_row, n_sorted)
        block_row = jnp.minimum(block_row, n_steps * ROWS - ALIGN)
        table_row = lax.broadcasted_iota(jnp.int32, (n_blocks, tokens), 0)
        sched_v[...] = jnp.where(
            table_row == 0, step_expert, jnp.where(table_row == 1, step_row // ALIGN, block_row // ALIGN))
        to_scalar = pltpu.make_async_copy(sched_v, sched, w_sem.at[8])
        to_scalar.start()

        place_s[...] = place
        row_id = lax.broadcasted_iota(jnp.int32, (n_sorted, tokens), 0)
        groups = (
            ((core, chip), (other, chip)), ((core, left), (core, right)), ((other, left), (other, right)),
            ((core, far), (other, far)))
        for n, pair in enumerate(groups):
            for m, (c, spot) in enumerate(pair):
                match = row_id == place_s[pl.ds(c * n_x + spot, 1), :]
                first_col = (2 * n + m) * tokens
                sort[:, first_col:first_col + tokens] = jnp.where(match, 1.0, 0.0).astype(BF16)

        def sort_weights():
            for k in range(1, n_ep):
                source = (ep + n_ep - k) % n_ep
                arrived(meta.at[(source % 2) * n_x + source // 2], m_recv.at[k - 1])
            weight = jnp.where(choice == 1, meta[:, 1, :], meta[:, 0, :])
            weight_rows = jnp.zeros((n_sorted, tokens), F32)
            for j in range(n_blocks):
                weight_rows = weight_rows + jnp.where(row_id == place[j:j + 1, :], weight[j:j + 1, :], 0.0)
            weight_sorted[0:n_sorted, :] = jnp.broadcast_to(
                jnp.sum(weight_rows, axis=1, keepdims=True), (n_sorted, 128))
            weight_sorted[n_sorted:, :] = jnp.zeros((ROWS, 128), F32)

        xs[n_sorted:, :] = jnp.zeros((ROWS, dim), BF16)
        def add_rows(n):
            def one(i, carry):
                cols = pl.ds(pl.multiple_of(i * 256, 256), 256)
                rows = jnp.concatenate([rows_all[c, spot, :, cols] for c, spot in groups[n]], axis=0)
                total = dot_nn(sort[:, 2 * n * tokens:(2 * n + 2) * tokens], rows)
                if n > 0:
                    total = total + xs[0:n_sorted, cols].astype(F32)
                xs[0:n_sorted, cols] = total.astype(BF16)
                return carry

            lax.fori_loop(0, dim // 256, one, 0, unroll=2)

        arrived(rows_all.at[other, chip], ag_recv.at[0])
        add_rows(0)
        along_y(5)
        along_y(6)
        for index in (1, 3, 2, 4):
            across(index)
        add_rows(1)
        for index in (5, 6):
            across(index)
        for k in range(1, n_tp):
            remote(part_q.at[(tp + k) % n_tp], part_in.at[k - 1], a_send.at[k - 1], a_recv.at[k - 1], tp_peer(k)).start()
        place_cols = jnp.transpose(place.astype(F32))
        column_id = lax.broadcasted_iota(jnp.int32, (tokens, n_sorted), 1).astype(F32)
        for j in range(n_blocks):
            unsort[j * tokens:(j + 1) * tokens, :] = jnp.where(
                column_id == place_cols[:, j:j + 1], 1.0, 0.0).astype(BF16)
        sort_weights()
        for index in (1, 3, 2, 4):
            arrived_across(index)
        add_rows(2)
        for index in (5, 6):
            arrived_across(index)
        add_rows(3)
        for index in messages:
            sent(rows_all.at[core, chip, low, side], ag_send.at[index])
            sent(rows_all.at[core, chip, low, side], y_send.at[index - 1])
            sent(rows_all.at[core, chip, low], ag_send.at[index + 6])
        sent(rows_all.at[core, chip], ag_send.at[0])
        for k in range(1, n_ep):
            sent(meta.at[core * n_x + chip], m_send.at[k - 1])
            sent(all_ids.at[core * n_x + chip], i_send.at[k - 1])
        to_scalar.wait()
        for e in range(n_local):
            pltpu.make_async_copy(eg_hbm.at[e], eg.at[e], e_sem.at[0, e]).wait()
            pltpu.make_async_copy(eu_hbm.at[e], eu.at[e], e_sem.at[1, e]).wait()

        def gate_up(step, carry):
            e = sched[0, step]
            rows = xs[pl.ds(sched[1, step] * ALIGN, ROWS), :]
            act = jax.nn.silu(dot_nt(eg[e], rows)) * dot_nt(eu[e], rows)
            z[step] = jnp.transpose(act).astype(BF16)
            return carry

        lax.fori_loop(0, n_steps, gate_up, 0, unroll=3)

        for p in range(dense_parts):
            pltpu.make_async_copy(wg_hbm.at[p], eg.at[p], w_sem.at[p]).start()
            pltpu.make_async_copy(wu_hbm.at[p], eu.at[p], w_sem.at[2 + p]).start()
            pltpu.make_async_copy(wd_hbm.at[p], eg.at[dense_parts + p], w_sem.at[4 + p]).start()
        for e in range(n_local):
            pltpu.make_async_copy(ed_hbm.at[e], ed.at[e], e_sem.at[2, e]).wait()

        def results(i):
            cols = columns(i)

            def down(step, carry):
                e = sched[0, step]
                scale = weight_sorted[pl.ds(sched[1, step] * ALIGN, ROWS), :]
                prod = dot_nn(z[step], ed[e, :, cols])
                scaled = [prod[:, b * 128:(b + 1) * 128] * scale for b in range(quarter // 128)]
                ys[pl.ds(pl.multiple_of(step * ROWS, ROWS), ROWS), :] = jnp.concatenate(scaled, axis=1).astype(BF16)
                return carry

            lax.fori_loop(0, n_steps, down, 0, unroll=9)

            def regroup(b, carry):
                y_sorted[pl.ds(pl.multiple_of(b * ALIGN, ALIGN), ALIGN), :] = ys[pl.ds(sched[2, b] * ALIGN, ALIGN), :]
                return carry

            lax.fori_loop(0, n_sorted // ALIGN, regroup, 0, unroll=8)

        def to_tokens(i):
            cols = columns(i)
            back = dot_nn(unsort[...], y_sorted[...])
            rows_all[:, :, :, cols] = back.astype(BF16).reshape(2, n_x, tokens, quarter)
            remote(rows_all.at[other, :, :, cols], d_in.at[i], d_send.at[i], d_recv.at[i], partner).start()

        attention_sum()
        results(0)
        to_tokens(0)
        results(1)
        pair_sum(0)
        pair_sum_rest(0)
        to_tokens(1)
        results(2)
        pair_sum(1)
        pair_sum_rest(1)
        to_tokens(2)
        ring_sum(0)
        results(3)
        pair_sum(2)
        pair_sum_rest(2)
        to_tokens(3)
        ring_sum(1)
        pair_sum(3)
        ring_sum(2)
        dense_gate_up(act_s)
        pair_sum_rest(3)
        dense_down(act_s)
        ring_sum(3)
        finish(0)
        finish(1)
        finish(2)
        finish(3)

    def columns(i):
        return pl.ds(pl.multiple_of(((tp + 1 + i) % n_tp) * quarter, quarter), quarter)

    def pair_sum(i):
        cols = columns(i)
        arrived(d_in.at[i], d_recv.at[i])
        for spot in range(n_x):
            rows_all[core, spot, :, cols] = (
                rows_all[core, spot, :, cols].astype(F32) + d_in[i, spot].astype(F32)).astype(BF16)
        remote(rows_all.at[core, far, low, cols], r1_in.at[i, 0], r1_send.at[i, 0], r1_recv.at[i, 0], on_ring(right)).start()
        remote(rows_all.at[core, far, high, cols], r1_in.at[i, 1], r1_send.at[i, 1], r1_recv.at[i, 1], on_ring(left)).start()

    def pair_sum_rest(i):
        cols = columns(i)
        remote(rows_all.at[core, right, high, cols], r2_in.at[i, 0, high], r2_send.at[i, 0], r2_recv.at[i, 0], on_ring(right)).start()
        remote(rows_all.at[core, left, low, cols], r2_in.at[i, 1, low], r2_send.at[i, 1], r2_recv.at[i, 1], on_ring(left)).start()

    def ring_sum(i):
        cols = columns(i)
        arrived(r1_in.at[i, 0], r1_recv.at[i, 0])
        rows_all[core, right, low, cols] = (
            rows_all[core, right, low, cols].astype(F32) + r1_in[i, 0].astype(F32)).astype(BF16)
        remote(rows_all.at[core, right, low, cols], r2_in.at[i, 0, low], r2_send.at[i, 2], r2_recv.at[i, 2], on_ring(right)).start()
        arrived(r1_in.at[i, 1], r1_recv.at[i, 1])
        rows_all[core, left, high, cols] = (
            rows_all[core, left, high, cols].astype(F32) + r1_in[i, 1].astype(F32)).astype(BF16)
        remote(rows_all.at[core, left, high, cols], r2_in.at[i, 1, high], r2_send.at[i, 3], r2_recv.at[i, 3], on_ring(left)).start()

    def dense_gate_up(act_s):
        for k in range(1, n_tp):
            source = (tp + n_tp - k) % n_tp
            arrived(h_q.at[source], h_recv.at[k - 1])
        hidden_mid = jnp.concatenate([h_q[q] for q in range(n_tp)], axis=1)
        c_buf[...] = rms_norm(hidden_mid, as_row(n_res_ref[...]))
        for p in range(dense_parts):
            pltpu.make_async_copy(wg_hbm.at[p], eg.at[p], w_sem.at[p]).wait()
            pltpu.make_async_copy(wu_hbm.at[p], eu.at[p], w_sem.at[2 + p]).wait()
            act = jax.nn.silu(dot_nt(eg[p], c_buf[...])) * dot_nt(eu[p], c_buf[...])
            act_s[p] = jnp.transpose(act).astype(BF16)

    def dense_down(act_s):
        for p in range(dense_parts):
            pltpu.make_async_copy(wd_hbm.at[p], eg.at[dense_parts + p], w_sem.at[4 + p]).wait()
        for q in range(n_tp):
            cols = slice(q * quarter, (q + 1) * quarter)
            dense = dot_nn(act_s[0], eg[dense_parts, :, cols])
            for p in range(1, dense_parts):
                dense = dense + dot_nn(act_s[p], eg[dense_parts + p, :, cols])
            dense_q[q] = dense

    def finish(i):
        q = (tp + 1 + i) % n_tp
        cols = columns(i)
        arrived(r2_in.at[i, 0, high], r2_recv.at[i, 0])
        arrived(r2_in.at[i, 1, low], r2_recv.at[i, 1])
        arrived(r2_in.at[i, 0, low], r2_recv.at[i, 2])
        arrived(r2_in.at[i, 1, high], r2_recv.at[i, 3])
        part = rows_all[core, chip, :, cols].astype(F32) + r2_in[i, 0].astype(F32) + r2_in[i, 1].astype(F32) + dense_q[q]
        if i < n_tp - 1:
            fin_q[i] = part.astype(BF16)
            remote(fin_q.at[i], fin_in.at[i], f_send.at[i], f_recv.at[i], tp_peer(i + 1)).start()
        else:
            for k in range(1, n_tp):
                arrived(fin_in.at[k - 1], f_recv.at[k - 1])
                part = part + fin_in[k - 1].astype(F32)
            out_q[tp] = (h_q[tp].astype(F32) + part).astype(BF16)

    pl.run_scoped(
        expert_phase,
        pltpu.VMEM((n_sorted + ROWS, dim), BF16),
        pltpu.VMEM((n_sorted, all_rows), BF16),
        pltpu.VMEM((all_rows, n_sorted), BF16),
        pltpu.VMEM((n_steps, ROWS, width), BF16),
        pltpu.VMEM((n_steps * ROWS, quarter), BF16),
        pltpu.VMEM((n_sorted, quarter), BF16),
        pltpu.VMEM((n_sorted + ROWS, 128), F32),
        pltpu.VMEM((n_blocks, tokens), jnp.int32),
        pltpu.VMEM((dense_parts, tokens, width), BF16),
    )
    before, after, opposite = (tp + n_tp - 1) % n_tp, (tp + 1) % n_tp, (tp + 2) % n_tp
    up, down = tp_peer(1), tp_peer(n_tp - 1)

    def pass_on(index, place, rows, device):
        block = out_q.at[place, rows]
        remote(block, block, o_send.at[index], o_recv.at[index], device).start()

    pass_on(0, tp, low, up)
    pass_on(1, tp, high, down)
    out_ref[:, pl.ds(pl.multiple_of(tp * quarter, quarter), quarter)] = out_q[tp]
    for index in range(2):
        sent(out_q.at[tp, low], o_send.at[index])
    pass_on(2, tp, high, up)
    pass_on(3, tp, low, down)
    arrived(out_q.at[before, low], o_recv.at[0])
    pass_on(4, before, low, up)
    arrived(out_q.at[after, high], o_recv.at[1])
    pass_on(5, after, high, down)

    for i in range(n_tp):
        cols = columns(i)
        sent(d_in.at[i], d_send.at[i])
        for side in range(2):
            sent(r1_in.at[i, side], r1_send.at[i, side])
        for message in range(4):
            sent(r1_in.at[i, 0], r2_send.at[i, message])
    for k in range(1, n_tp):
        sent(part_in.at[k - 1], a_send.at[k - 1])
        sent(part_in.at[k - 1], h_send.at[k - 1])
        sent(part_in.at[k - 1], f_send.at[k - 1])
    arrived(out_q.at[before, high], o_recv.at[2])
    arrived(out_q.at[after, low], o_recv.at[3])
    for place in (before, after):
        out_ref[:, pl.ds(pl.multiple_of(place * quarter, quarter), quarter)] = out_q[place]
    arrived(out_q.at[opposite, low], o_recv.at[4])
    arrived(out_q.at[opposite, high], o_recv.at[5])
    out_ref[:, pl.ds(pl.multiple_of(opposite * quarter, quarter), quarter)] = out_q[opposite]
    for index in range(2, 6):
        sent(out_q.at[tp, low], o_send.at[index])


def cache_kernel(pieces, pos, hidden, k_new_hbm, v_new_hbm, k_hbm, v_hbm, out, k_out, v_out, hidden_buf, k_new, v_new, k_buf, v_buf, in_sem, out_sem, sem):
    size = k_buf.shape[0] // pieces
    both = ((k_hbm, k_buf, k_out, k_new), (v_hbm, v_buf, v_out, v_new))
    first = [
        pltpu.make_async_copy(k_new_hbm, k_new, sem.at[0]),
        pltpu.make_async_copy(v_new_hbm, v_new, sem.at[1]),
    ]
    hidden_in, hidden_out = (
        pltpu.make_async_copy(hidden, hidden_buf, sem.at[2]), pltpu.make_async_copy(hidden_buf, out, sem.at[3]))
    loads = [
        [pltpu.make_async_copy(src.at[pl.ds(i * size, size)], buf.at[pl.ds(i * size, size)], in_sem.at[n, i])
         for n, (src, buf, _, _) in enumerate(both)] for i in range(pieces)]
    stores = [
        [pltpu.make_async_copy(buf.at[pl.ds(i * size, size)], dst.at[pl.ds(i * size, size)], out_sem.at[n, i])
         for n, (_, buf, dst, _) in enumerate(both)] for i in range(pieces)]
    for load in first:
        load.start()
    for pair in loads:
        for load in pair:
            load.start()
    hidden_in.start()
    for load in first:
        load.wait()
    for i in range(pieces):
        for n, (_, buf, _, new) in enumerate(both):
            loads[i][n].wait()
            for t in range(i * size, (i + 1) * size):
                buf[t, pos[t]] = new[t]
            stores[i][n].start()
    hidden_in.wait()
    hidden_out.start()
    for pair in stores:
        for store in pair:
            store.wait()
    hidden_out.wait()


def rope_table(cache_len, head_dim):
    freq = 1.0 / (ROPE_BASE ** (np.arange(0, head_dim, 2, dtype=np.float32) / np.float32(head_dim)))
    angle = np.arange(cache_len, dtype=np.float32)[:, None] * freq.astype(np.float32)[None, :]
    cosine, sine = np.cos(angle), np.sin(angle)
    return np.concatenate(
        [np.concatenate([cosine, cosine], 1), np.concatenate([-sine, sine], 1)], 0).astype(np.float32)


def solution(mesh):
    n_tp, n_ep = mesh.shape['tp'], mesh.shape['ep']
    row_spec = P(('dp', 'ep'), None)
    cache_spec = P(('dp', 'ep'), None, 'tp', None)
    col_split = P(None, 'tp')
    row_split = P('tp', None)
    in_specs = (row_spec, P(('dp', 'ep')), row_spec, cache_spec, cache_spec, P(None), P(None), P(None), col_split, col_split, col_split, row_split, col_split, col_split, row_split, P(None, None), P('ep', None, 'tp'), P('ep', None, 'tp'), P('ep', 'tp', None))
    out_specs = (row_spec, cache_spec, cache_spec)

    def local_layer(hidden_in, positions, expert_ids, k_cache, v_cache, norm_in, norm_res, norm_post, w_q, w_k, w_v, w_o, w_gate, w_up, w_down, w_router, e_gate, e_up, e_down):
        tokens, dim = hidden_in.shape
        n_local, width = e_gate.shape[0], e_gate.shape[2]
        cache_len, heads, head_dim = k_cache.shape[1:]
        dense_parts = w_down.shape[0] // width
        quarter = dim // n_tp
        n_x = n_ep // 2
        half = tokens // 2
        vmem = pl.BlockSpec(memory_space=pltpu.VMEM)
        hbm = pl.BlockSpec(memory_space=pl.ANY)
        dma = pltpu.SemaphoreType.DMA
        hidden, k_new, v_new = pl.pallas_call(
            functools.partial(layer_kernel, n_tp, n_ep, 'ep', 'tp'),
            out_shape=(
                jax.ShapeDtypeStruct(hidden_in.shape, BF16),
                jax.ShapeDtypeStruct((tokens * heads, head_dim), BF16),
                jax.ShapeDtypeStruct((tokens * heads, head_dim), BF16),
            ),
            in_specs=[vmem] * 8 + [hbm] * 12,
            out_specs=(vmem, vmem, vmem),
            scratch_shapes=[
                pltpu.VMEM((n_local, width, dim), BF16),
                pltpu.VMEM((n_local, width, dim), BF16),
                pltpu.VMEM((n_local, width, dim), BF16),
                pltpu.VMEM((2, n_x, tokens, dim), BF16),
                pltpu.VMEM((n_ep, 8, tokens), F32),
                pltpu.VMEM((n_ep, 8, tokens), jnp.int32),
                pltpu.VMEM((n_tp, tokens, quarter), BF16),
                pltpu.VMEM((n_tp - 1, tokens, quarter), BF16),
                pltpu.VMEM((n_tp, tokens, quarter), BF16),
                pltpu.VMEM((tokens, dim), BF16),
                pltpu.VMEM((n_tp, n_x, tokens, quarter), BF16),
                pltpu.VMEM((n_tp, 2, half, quarter), BF16),
                pltpu.VMEM((n_tp, 2, tokens, quarter), BF16),
                pltpu.VMEM((n_tp, tokens, quarter), F32),
                pltpu.VMEM((n_tp - 1, tokens, quarter), BF16),
                pltpu.VMEM((n_tp - 1, tokens, quarter), BF16),
                pltpu.VMEM((n_tp, tokens, quarter), BF16),
                pltpu.VMEM((n_ep, tokens), jnp.int32),
                pltpu.SMEM((n_ep, tokens), jnp.int32),
                dma((9,)), dma((3, n_local)), dma((13,)), dma((13,)), *[dma((n_ep - 1,))] * 4, dma((6,)), dma((6,)),
                *[dma((n_tp - 1,))] * 4,
                dma((n_tp,)), dma((n_tp,)),
                dma((n_tp, 2)), dma((n_tp, 2)), dma((n_tp, 4)), dma((n_tp, 4)),
                *[dma((n_tp - 1,))] * 2, dma((6,)), dma((6,)),
            ],
            compiler_params=pltpu.CompilerParams(
                collective_id=0, has_side_effects=True, vmem_limit_bytes=67043328),
        )(
            hidden_in, positions.reshape(1, tokens), expert_ids.T,
            norm_in.reshape(-1, 128), norm_res.reshape(-1, 128), norm_post.reshape(-1, 128), w_router.T,
            jnp.asarray(rope_table(cache_len, head_dim)),
            k_cache.reshape(-1, head_dim), v_cache.reshape(-1, head_dim), w_q, w_k, w_v, w_o,
            w_gate.T.reshape(dense_parts, width, dim), w_up.T.reshape(dense_parts, width, dim),
            w_down.reshape(dense_parts, width, dim),
            jnp.swapaxes(e_gate, 1, 2), jnp.swapaxes(e_up, 1, 2), e_down,
        )
        return pl.pallas_call(
            functools.partial(cache_kernel, 8),
            out_shape=(
                jax.ShapeDtypeStruct(hidden_in.shape, BF16),
                jax.ShapeDtypeStruct(k_cache.shape, BF16),
                jax.ShapeDtypeStruct(v_cache.shape, BF16),
            ),
            in_specs=[pl.BlockSpec(memory_space=pltpu.SMEM)] + [hbm] * 5,
            out_specs=(hbm, hbm, hbm),
            scratch_shapes=[
                pltpu.VMEM(hidden_in.shape, BF16),
                pltpu.VMEM((tokens, heads, head_dim), BF16), pltpu.VMEM((tokens, heads, head_dim), BF16),
                pltpu.VMEM(k_cache.shape, BF16), pltpu.VMEM(v_cache.shape, BF16),
                dma((2, 8)), dma((2, 8)), dma((4,)),
            ],
        )(positions, hidden, k_new.reshape(tokens, heads, head_dim), v_new.reshape(tokens, heads, head_dim), k_cache, v_cache)

    return jax.shard_map(local_layer, mesh=mesh, in_specs=in_specs, out_specs=out_specs, check_vma=False)
```
